256 devices in a mesh: groups: 2 (over z), section: 64 (over y, x), head: 2 (over core).
Axes of the slice: x: 8, y: 8, z: 2, core: 2. Of those that a mesh axis runs over, the one named last changes fastest.
The devices are a block of a 8x8x16 slice.
Arguments:
- video_tokens: bfloat16 [65536, 1536], P(('groups', 'section', 'head')), parts along dimension 0, may hold values from -6 to 6
- modulation: float32 [6, 1536], P('groups'), parts along dimension 0, may hold values from -3 to 3
- project_weight: bfloat16 [3, 1536, 1536], P(None, None, 'head'), may hold values from -0.15625 to 0.15625
- output_weight: bfloat16 [1536, 1536], P('head'), may hold values from -0.15625 to 0.15625
- norm_gains: float32 [3, 128], replicated, may hold values from 1 to 2
- text_cache: bfloat16 [2, 512, 1536], P(None, 'groups', 'head'), parts along dimension 1, may hold values from -6 to 6
- text_count: int32 [2], P('groups'), parts along dimension 0, may hold values from 1 to 256, as said below
- video_keep: int32 [65536], P('groups'), parts along dimension 0, may hold values 0 or 1
- patch_order: int32 [128], P('groups'), parts along dimension 0, may hold values from 0 to 63, each once
- stale_cache: bfloat16 [2, 65536, 1536], P(None, ('groups', 'section'), 'head'), parts along dimension 1, may hold values from -6 to 6
Outputs:
- updated: bfloat16 [65536, 1536], P(('groups', 'section', 'head')), parts along dimension 0
- fresh_cache: bfloat16 [2, 65536, 1536], P(None, ('groups', 'section'), 'head'), parts along dimension 1
The draws below stay inside these ranges and needn't reach their ends.
There are 2 independent parts, one for each index of `groups`. The reference program is written for one: setup_inputs(seed, part) draws one part's arguments, and reference() takes and returns one part's arrays. A program takes and returns all parts, laid end to end along the dimension named above; an argument that names none is the same for every part. Nothing has to cross between parts.
Inputs may be any that keep to these rules, and one draw needn't show every extreme that they name: The first text_count text tokens are real, the rest are padding. `video_keep`: 1 keeps a video token as a key, 0 marks padding. `patch_order`: each place 0 to 63 is held by exactly one patch.
All inputs are finite; a program needn't handle non-finite values.
Results may differ from the reference program's by a relative error of at most 0.0049.
Values may be sent and summed in bfloat16 or wider, within the bound.
A program may use at most 128 MiB of HBM per device.

```python
import jax
import jax.numpy as jnp
from jax import lax

D = 1536
HEADS = 12
HEAD_DIM = 128
TEXT = 256
PATCH = 512
HID = 1536
SEQ = 32768
N_SECTION = 64


def draw_text_count(key, part):
    short = jax.random.randint(key, (1,), 1, TEXT // 2 + 1, dtype=jnp.int32)
    odd_part = jnp.asarray(part, jnp.int32) % 2 == 1
    return jnp.where(odd_part, jnp.full((1,), TEXT, jnp.int32), short).astype(jnp.int32)


def with_ends(entries, key, low, top_value):
    extent = entries.shape
    place = [jax.random.randint(jax.random.fold_in(key, axis), (), 0, extent[axis]) for axis in range(len(extent))]
    entries = entries.at[tuple(place)].set(low)
    longest = extent.index(max(extent))
    place[longest] = (place[longest] + 1) % extent[longest]
    return entries.at[tuple(place)].set(top_value)


def block_levels(own_key, dims, cuts, least, largest):
    loudness = 1.0
    for position, blocks in cuts:
        steps = jax.random.uniform(jax.random.fold_in(jax.random.fold_in(own_key, 6), position), (blocks,), jnp.float32, least / len(cuts), largest / len(cuts))
        loudness = loudness * jnp.repeat(jnp.exp(steps), dims[position] // blocks).reshape((-1,) + (1,) * (len(dims) - 1 - position))
    return loudness


def normal_values(rng, dims, deviation, most, split=(), kind=jnp.bfloat16):
    result = deviation * jax.random.normal(rng, dims, jnp.float32)
    if split:
        result = result * block_levels(rng, dims, split, -0.22, 0.18)
    return jnp.clip(result, -most, most).astype(kind)


def setup_inputs(seed: int = 0, part: int = 0) -> dict:
    streams_of = jax.random.split(jax.random.key(seed), 11)
    own_keys = jax.random.split(jax.random.fold_in(streams_of[10], part), 11)
    video_tokens = normal_values(own_keys[0], (SEQ, D), 1.0, 6.0, ((0, 128),))
    modulation = normal_values(own_keys[1], (3, D), 0.7, 3.0, (), jnp.float32)
    project_weight = normal_values(streams_of[2], (3, D, HID), D ** -0.5, 0.15625, ((2, 2),))
    output_weight = normal_values(streams_of[3], (HID, D), HID ** -0.5, 0.15625, ((0, 2),))
    norm_gains = jnp.clip(jax.random.uniform(streams_of[4], (3, HEAD_DIM), jnp.float32, 1.0, 2.0), 1.0, 2.0)
    text_cache = normal_values(own_keys[5], (2, TEXT, HID), 1.4, 6.0, ((2, 2),))
    text_count = draw_text_count(jax.random.fold_in(jax.random.fold_in(streams_of[10], part), 71), part)
    video_keep = with_ends((jax.random.randint(own_keys[7], (SEQ,), 0, 4) < 3).astype(jnp.int32), jax.random.fold_in(own_keys[7], 1), 0, 1)
    patch_order = jax.random.permutation(own_keys[8], N_SECTION).astype(jnp.int32)
    stale_cache = normal_values(own_keys[9], (2, SEQ, HID), 1.4, 6.0, ((1, 64), (2, 2)))
    return dict(video_tokens=video_tokens, modulation=modulation, project_weight=project_weight, output_weight=output_weight, norm_gains=norm_gains, text_cache=text_cache, text_count=text_count, video_keep=video_keep, patch_order=patch_order, stale_cache=stale_cache)


epsilon = 1e-06

def widen(array):
    return lax.optimization_barrier(array).astype(jnp.float32)

def layer_norm(values):
    center = lax.optimization_barrier(jnp.mean(values, axis=-1, keepdims=True))
    shifted = values - center
    spread = lax.optimization_barrier(jnp.mean(shifted * shifted, axis=-1, keepdims=True))
    return shifted * lax.rsqrt(spread + epsilon)

def head_norm(inputs, gain_row):
    per_head = inputs.reshape(inputs.shape[0], HEADS, HEAD_DIM)
    scaled = per_head * lax.rsqrt(lax.optimization_barrier(jnp.mean(per_head * per_head, axis=-1, keepdims=True)) + epsilon) * gain_row
    return scaled.astype(jnp.bfloat16)

def reference(video_tokens, modulation, project_weight, output_weight, norm_gains, text_cache, text_count, video_keep, patch_order, stale_cache):
    hidden = video_tokens.astype(jnp.float32)
    normed = (layer_norm(hidden) * (1.0 + modulation[1]) + modulation[0]).astype(jnp.bfloat16)
    projected = jnp.einsum('sd,cdh->csh', widen(normed), project_weight.astype(jnp.float32), precision=lax.Precision.HIGHEST)
    fresh_cache = projected[1:3].astype(jnp.bfloat16)
    queries = head_norm(projected[0], norm_gains[0])
    fresh_keys = head_norm(widen(fresh_cache[0]), norm_gains[1])
    stale_keys = head_norm(stale_cache[0].astype(jnp.float32), norm_gains[1])
    text_keys = head_norm(text_cache[0].astype(jnp.float32), norm_gains[2])
    fresh_values = fresh_cache[1].reshape(SEQ, HEADS, HEAD_DIM)
    stale_values = stale_cache[1].reshape(SEQ, HEADS, HEAD_DIM)
    text_values = text_cache[1].reshape(TEXT, HEADS, HEAD_DIM)
    text_live = jnp.arange(TEXT, dtype=jnp.int32) < text_count[0]
    score_scale = HEAD_DIM ** (-0.5)

    def rows_of(array, patch_index):
        return lax.dynamic_slice_in_dim(array, (patch_index * PATCH).astype(jnp.int32), PATCH, 0)

    def one_patch(patch_index):
        left_place = jnp.maximum(patch_index - 1, 0).astype(jnp.int32)
        right_place = jnp.minimum(patch_index + 1, N_SECTION - 1).astype(jnp.int32)
        own_slot = patch_order[patch_index]
        left_fresh = patch_order[left_place] < own_slot
        right_fresh = patch_order[right_place] < own_slot
        left_keys = jnp.where(left_fresh, rows_of(fresh_keys, left_place), rows_of(stale_keys, left_place))
        right_keys = jnp.where(right_fresh, rows_of(fresh_keys, right_place), rows_of(stale_keys, right_place))
        left_values = jnp.where(left_fresh, rows_of(fresh_values, left_place), rows_of(stale_values, left_place))
        right_values = jnp.where(right_fresh, rows_of(fresh_values, right_place), rows_of(stale_values, right_place))
        key_rows = jnp.concatenate([left_keys, rows_of(fresh_keys, patch_index), right_keys, text_keys], axis=0)
        value_rows = jnp.concatenate([left_values, rows_of(fresh_values, patch_index), right_values, text_values], axis=0)
        key_live = jnp.concatenate([(rows_of(video_keep, left_place) > 0) & (patch_index > 0), rows_of(video_keep, patch_index) > 0, (rows_of(video_keep, right_place) > 0) & (patch_index < N_SECTION - 1), text_live])
        query_rows = rows_of(queries, patch_index)
        scores = jnp.einsum('qhd,khd->hqk', query_rows.astype(jnp.float32), key_rows.astype(jnp.float32), precision=lax.Precision.HIGHEST) * score_scale
        weights = jnp.where(key_live[None, None, :], jnp.exp(scores), 0.0)
        total = lax.optimization_barrier(jnp.sum(weights, axis=-1))
        numerator = jnp.einsum('hqk,khd->qhd', widen(weights.astype(jnp.bfloat16)), value_rows.astype(jnp.float32), precision=lax.Precision.HIGHEST)
        return (numerator / jnp.transpose(total)[:, :, None]).astype(jnp.bfloat16).reshape(PATCH, HID)
    attended = lax.map(one_patch, jnp.arange(N_SECTION, dtype=jnp.int32)).reshape(SEQ, HID)
    mixed = jnp.dot(attended, output_weight, preferred_element_type=jnp.float32)
    updated = (hidden + modulation[2] * mixed).astype(jnp.bfloat16)
    return (updated, fresh_cache)
```

```python
import functools
import math

import jax
import jax.numpy as jnp
from jax import lax
from jax.experimental import pallas as pl
from jax.experimental.pallas import tpu as pltpu
from jax.sharding import PartitionSpec as P

epsilon = 1e-06
CHUNKS = 4
F32 = jnp.float32
BF16 = jnp.bfloat16
MESH = pl.DeviceIdType.MESH
NT = (((1,), (1,)), ((), ()))


def matmul(a, b):
    return jnp.dot(a, b, preferred_element_type=F32)


def head_norm(values, gain):
    square = jnp.mean(values * values, axis=-1, keepdims=True)
    return values * lax.rsqrt(square + epsilon) * gain


def kernel(
    order_s, count_s, x_h, mod_h, w_h, wo_h, gains_h, text_h, keep_h, stale_h,
    updated_h, fresh_h,
    x_v, mod_v, w_v, wo_v, gains_v, text_v, keep_v, stale_v,
    normed, message, arrived, fresh_v, q_own, kbuf, vbuf, mbuf, kst, vst, nq, acc,
    r_out, r_in, t_out, t_in, attended, y_out, y_in, upd_v,
    load_sem, part_send, part_recv, p1_send, p1_recv, f_send, f_recv,
    r_send, r_recv, t_send, t_recv, y_send, y_recv, out_sem, fresh_sem,
):
    rows, width = x_v.shape
    patch, local = stale_v.shape[1], stale_v.shape[2]
    text_rows = text_v.shape[1]
    hd = gains_v.shape[1]
    heads = local // hd
    half_heads = heads // 2
    half = half_heads * hd
    sub = rows // CHUNKS
    keys = 4 * sub
    own_chunks = patch // keys
    sections = lax.axis_size("section")
    place = lax.axis_index("section")
    h = lax.axis_index("head")
    right = lax.rem(place + 1, sections)
    left = lax.rem(place + sections - 1, sections)
    nbr_of = ({"section": left}, {"section": right})
    partner = {"head": 1 - h}

    loads = [
        pltpu.make_async_copy(src, dst, load_sem.at[i])
        for i, (src, dst) in enumerate(
            [
                (x_h, x_v), (mod_h, mod_v), (stale_h, stale_v), (gains_h, gains_v), (keep_h, keep_v),
                (text_h, text_v), (w_h, w_v), (wo_h, wo_v),
            ]
        )
    ]
    for load in loads:
        load.start()

    barrier = pltpu.get_barrier_semaphore()
    for device in (nbr_of[0], nbr_of[1], partner):
        pl.semaphore_signal(barrier, inc=1, device_id=device, device_id_type=MESH)

    own_slot = order_s[place]
    slot = (order_s[left], order_s[right])
    exists = (place > 0, place < sections - 1)
    one = jnp.int32(1)
    zero = jnp.int32(0)
    is_b = [jnp.where(slot[n] < own_slot, one, zero) * jnp.where(exists[n], one, zero) for n in range(2)]
    is_a = [jnp.where(slot[n] > own_slot, one, zero) * jnp.where(exists[n], one, zero) for n in range(2)]
    gives = [jnp.where(own_slot < slot[n], one, zero) for n in range(2)]

    def full(flag, shape):
        return jnp.full(shape, flag, jnp.int32) > 0

    for i in (0, 1, 2):
        loads[i].wait()
    scale = 1.0 + mod_v[1:2, :]
    shift = mod_v[0:1, :]
    base = pl.multiple_of(h * rows, rows)

    def p1_copy(n, c):
        at = pl.ds(pl.multiple_of((1 - n) * 2 * sub + h * sub, sub), sub)
        return pltpu.make_async_remote_copy(
            src_ref=message.at[n, pl.ds(c * sub, sub), :],
            dst_ref=arrived.at[c, at, :],
            send_sem=p1_send.at[n, c],
            recv_sem=p1_recv.at[1 - n, c],
            device_id=nbr_of[n],
            device_id_type=MESH,
        )

    def p1_wait(n, c):
        at = pl.ds(pl.multiple_of(n * 2 * sub + h * sub, sub), sub)
        return pltpu.make_async_remote_copy(
            src_ref=message.at[n, pl.ds(c * sub, sub), :],
            dst_ref=arrived.at[c, at, :],
            send_sem=p1_send.at[n, c],
            recv_sem=p1_recv.at[n, c],
            device_id=nbr_of[n],
            device_id_type=MESH,
        )

    def part_copy(c):
        at = pl.ds(pl.multiple_of(base + c * sub, sub), sub)
        return pltpu.make_async_remote_copy(
            src_ref=normed.at[at, :],
            dst_ref=normed.at[at, :],
            send_sem=part_send.at[c],
            recv_sem=part_recv.at[c],
            device_id=partner,
            device_id_type=MESH,
        )

    def forward_copy(n, c):
        at = pl.ds(pl.multiple_of(n * 2 * sub + h * sub, sub), sub)
        return pltpu.make_async_remote_copy(
            src_ref=arrived.at[c, at, :],
            dst_ref=arrived.at[c, at, :],
            send_sem=f_send.at[n, c],
            recv_sem=f_recv.at[n, c],
            device_id=partner,
            device_id_type=MESH,
        )

    def r_copy(n, c):
        return pltpu.make_async_remote_copy(
            src_ref=r_out.at[n, c],
            dst_ref=r_in.at[1 - n, c],
            send_sem=r_send.at[n, c],
            recv_sem=r_recv.at[1 - n, c],
            device_id=nbr_of[n],
            device_id_type=MESH,
        )

    def t_copy(n, c):
        return pltpu.make_async_remote_copy(
            src_ref=t_out.at[n, c],
            dst_ref=t_in.at[1 - n, c],
            send_sem=t_send.at[n, c],
            recv_sem=t_recv.at[1 - n, c],
            device_id=nbr_of[n],
            device_id_type=MESH,
        )

    for c in range(CHUNKS):
        at = slice(c * sub, (c + 1) * sub)
        hidden = x_v[at, :].astype(F32)
        center = jnp.mean(hidden, axis=-1, keepdims=True)
        shifted = hidden - center
        spread = jnp.mean(shifted * shifted, axis=-1, keepdims=True)
        tokens = (shifted * lax.rsqrt(spread + epsilon) * scale + shift).astype(BF16)
        normed[pl.ds(pl.multiple_of(base + c * sub, sub), sub), :] = tokens
        other = slice(rows + c * sub, rows + (c + 1) * sub)
        packed = jnp.concatenate(
            [stale_v[0, at, half:], stale_v[0, other, half:], stale_v[1, at, half:], stale_v[1, other, half:]], axis=1
        )
        for n in range(2):
            message[n, at, :] = jnp.where(full(gives[n], tokens.shape), tokens, packed)
        if c == 0:
            pl.semaphore_wait(barrier, 3)
        for n in (1, 0):
            p1_copy(n, c).start()
        part_copy(c).start()

    for i in (3, 4, 5):
        loads[i].wait()

    def keep_column(index, part):
        row = keep_v[pl.ds(index * (patch // hd) + part, 1), :]
        return jnp.transpose(jnp.broadcast_to(row.astype(F32), (hd, hd)))

    for part in range(patch // hd):
        column = keep_column(place, part).astype(BF16)
        for group in range(2):
            mbuf[group, part * hd : (part + 1) * hd, :] = column
    live = lax.broadcasted_iota(jnp.int32, (text_rows, hd), 0) < count_s[0]
    text_mask = jnp.where(live, 1.0, 0.0).astype(BF16)
    for group in range(2):
        mbuf[group, patch : patch + text_rows, :] = text_mask
    for n in range(2):
        for part in range(patch // hd):
            column = keep_column((left, right)[n], part)
            seen = (
                jnp.where(full(is_b[n], column.shape), column, 0.0),
                jnp.where(full(is_a[n] + is_b[n], column.shape), column, 0.0),
            )
            for piece in range(hd // sub):
                row = part * hd + piece * sub
                core, c = row // rows, (row % rows) // sub
                to = patch + text_rows + c * keys + n * 2 * sub + core * sub
                for group in range(2):
                    mbuf[group, to : to + sub, :] = seen[group][piece * sub : (piece + 1) * sub].astype(BF16)

    q_gain = gains_v[0:1, :] * (math.log2(math.e) * hd**-0.5)
    k_gain = gains_v[1:2, :]
    t_gain = gains_v[2:3, :]

    for i in range(heads):
        cols = slice(i * hd, (i + 1) * hd)
        kbuf[patch : patch + text_rows, cols] = head_norm(text_v[0, :, cols].astype(F32), t_gain).astype(BF16)
        vbuf[patch : patch + text_rows, cols] = text_v[1, :, cols] * text_mask
    for i in range(half_heads):
        cols = slice(i * hd, (i + 1) * hd)
        kst[:, cols] = head_norm(stale_v[0, :, cols].astype(F32), k_gain).astype(BF16)
        vst[:, cols] = stale_v[1, :, cols] * mbuf[0, :patch, :]

    loads[6].wait()
    wide = 2 * hd

    def project_own(step, carry):
        side = lax.rem(h + step, 2)
        at = pl.ds(pl.multiple_of(side * rows, rows), rows)

        @pl.when(step == 1)
        def _():
            for c in range(CHUNKS):
                spot = pl.ds(pl.multiple_of(side * rows + c * sub, sub), sub)
                pltpu.make_async_remote_copy(
                    src_ref=normed.at[spot, :],
                    dst_ref=normed.at[spot, :],
                    send_sem=part_send.at[c],
                    recv_sem=part_recv.at[c],
                    device_id=partner,
                    device_id_type=MESH,
                ).wait_recv()

        for i in range(local // wide):
            block = slice(i * wide, (i + 1) * wide)
            keys_raw = matmul(normed[at, :], w_v[1, :, block]).astype(BF16)
            fresh_v[0, at, block] = keys_raw
            values_raw = matmul(normed[at, :], w_v[2, :, block]).astype(BF16)
            fresh_v[1, at, block] = values_raw
            queries = matmul(normed[at, :], w_v[0, :, block])
            for j in range(2):
                lanes = slice(j * hd, (j + 1) * hd)
                cols = slice(i * wide + j * hd, i * wide + (j + 1) * hd)
                kbuf[at, cols] = head_norm(keys_raw[:, lanes].astype(F32), k_gain).astype(BF16)
                vbuf[at, cols] = values_raw[:, lanes] * mbuf[0, at, :]
                q_own[at, cols] = head_norm(queries[:, lanes], q_gain).astype(BF16)
        pltpu.make_async_copy(fresh_v.at[:, at, :], fresh_h.at[:, at, :], fresh_sem.at[step]).start()
        return carry

    lax.fori_loop(0, 2, project_own, 0)

    def group_of(i):
        return 0 if i < half_heads else 1

    for i in range(heads):
        cols = slice(i * hd, (i + 1) * hd)
        score = lax.dot_general(q_own[:, cols], kbuf[:patch, cols], NT, preferred_element_type=F32)
        weight = jnp.exp2(score).astype(BF16)
        acc[i] = matmul(weight, jnp.concatenate([vbuf[:patch, cols], mbuf[0, :patch, :]], axis=1))

    def attend(chunk):
        at = pl.ds(pl.multiple_of(chunk * keys, keys), keys)
        for i in range(heads):
            cols = slice(i * hd, (i + 1) * hd)
            score = lax.dot_general(q_own[:, cols], kbuf[at, cols], NT, preferred_element_type=F32)
            weight = jnp.exp2(score).astype(BF16)
            acc[i] += matmul(weight, jnp.concatenate([vbuf[at, cols], mbuf[group_of(i), at, :]], axis=1))

    first = own_chunks + text_rows // keys

    def neighbours(c, carry):
        for n in range(2):
            p1_wait(n, c).wait_recv()
            forward_copy(n, c).start()
        attend(first - 1 + c)
        for n in range(2):
            at = pl.ds(pl.multiple_of(n * 2 * sub + (1 - h) * sub, sub), sub)
            pltpu.make_async_remote_copy(
                src_ref=arrived.at[c, at, :],
                dst_ref=arrived.at[c, at, :],
                send_sem=f_send.at[n, c],
                recv_sem=f_recv.at[n, c],
                device_id=partner,
                device_id_type=MESH,
            ).wait_recv()
        for i in range(half_heads):
            cols = slice(i * hd, (i + 1) * hd)
            nq[:, cols] = head_norm(matmul(arrived[c], w_v[0, :, cols]), q_gain).astype(BF16)
        for i in range(half_heads):
            cols = slice(i * hd, (i + 1) * hd)
            score = lax.dot_general(nq[:, cols], kst[:, cols], NT, preferred_element_type=F32)
            weight = jnp.exp2(score).astype(BF16)
            both = matmul(weight, jnp.concatenate([vst[:, cols], mbuf[0, :patch, :]], axis=1))
            for n in range(2):
                part = slice(n * 2 * sub, (n + 1) * 2 * sub)
                r_out[n, c, :, cols] = both[part, :hd].astype(BF16)
                t_out[n, c, i : i + 1, :] = jnp.transpose(both[part, hd:])[0:1, :]
        for n in range(2):
            r_copy(n, c).start()
            t_copy(n, c).start()
        to = pl.multiple_of((first + c) * keys, keys)
        for i in range(local // wide):
            block = slice(i * wide, (i + 1) * wide)
            keys_raw = matmul(arrived[c], w_v[1, :, block]).astype(BF16)
            values_raw = matmul(arrived[c], w_v[2, :, block]).astype(BF16)
            for j in range(2):
                head = 2 * i + j
                lanes = slice(j * hd, (j + 1) * hd)
                cols = slice(head * hd, (head + 1) * hd)
                for n in range(2):
                    part = slice(n * 2 * sub, (n + 1) * 2 * sub)
                    k_part, v_part = keys_raw[part, lanes], values_raw[part, lanes]
                    if group_of(head) == 1:
                        spot = pl.ds(pl.multiple_of(n * 2 * sub + h * sub, sub), sub)
                        off = (head - half_heads) * hd

                        def sent(index):
                            low = index * half + off
                            return jnp.concatenate(
                                [
                                    arrived[c, spot, low : low + hd],
                                    arrived[c, spot, low + half : low + half + hd],
                                ],
                                axis=0,
                            )

                        pick = full(is_b[n], k_part.shape)
                        k_part = jnp.where(pick, k_part, sent(0))
                        v_part = jnp.where(pick, v_part, sent(2))
                    spot_to = pl.ds(pl.multiple_of(to + n * 2 * sub, 2 * sub), 2 * sub)
                    kbuf[spot_to, cols] = head_norm(k_part.astype(F32), k_gain).astype(BF16)
                    vbuf[spot_to, cols] = v_part * mbuf[group_of(head), spot_to, :]
        return carry

    lax.fori_loop(0, CHUNKS, neighbours, 0)
    attend(first + CHUNKS - 1)

    for i in range(half_heads, heads):
        cols = slice(i * hd, (i + 1) * hd)
        attended[:, cols] = (acc[i, :, :hd] / acc[i, :, hd:]).astype(BF16)

    def combine(c, carry):
        for n in range(2):
            r_copy(1 - n, c).wait_recv()
            t_copy(1 - n, c).wait_recv()
        for i in range(half_heads):
            cols = slice(i * hd, (i + 1) * hd)
            spots = [pl.ds(pl.multiple_of(core * rows + c * sub, sub), sub) for core in range(2)]
            top = jnp.concatenate([acc[i, spot, :hd] for spot in spots], axis=0)
            low = jnp.concatenate([acc[i, spot, hd:] for spot in spots], axis=0)
            for n in range(2):
                pick = full(is_a[n], top.shape)
                total = jnp.transpose(jnp.broadcast_to(t_in[n, c, i : i + 1, :], (hd, 2 * sub)))
                top += jnp.where(pick, r_in[n, c, :, cols].astype(F32), 0.0)
                low += jnp.where(pick, total, 0.0)
            result = (top / low).astype(BF16)
            for core in range(2):
                attended[spots[core], cols] = result[core * sub : (core + 1) * sub]
        return carry

    lax.fori_loop(0, CHUNKS, combine, 0)

    loads[7].wait()
    steps = y_send.shape[0]
    span = width // steps
    other = pl.ds(pl.multiple_of((1 - h) * rows, rows), rows)
    mine = pl.ds(base, rows)

    def y_copy(s):
        cols = pl.ds(pl.multiple_of(s * span, span), span)
        return pltpu.make_async_remote_copy(
            src_ref=y_out.at[:, cols],
            dst_ref=y_in.at[:, cols],
            send_sem=y_send.at[s],
            recv_sem=y_recv.at[s],
            device_id=partner,
            device_id_type=MESH,
        )

    def send_part(s, carry):
        cols = pl.ds(pl.multiple_of(s * span, span), span)
        y_out[:, cols] = matmul(attended[other, :], wo_v[:, cols]).astype(BF16)
        y_copy(s).start()
        return carry

    lax.fori_loop(0, steps, send_part, 0)

    def out_copy(s):
        cols = pl.ds(pl.multiple_of(s * span, span), span)
        return pltpu.make_async_copy(upd_v.at[:, cols], updated_h.at[:, cols], out_sem.at[s])

    def finish(s, carry):
        cols = pl.ds(pl.multiple_of(s * span, span), span)
        mixed = matmul(attended[mine, :], wo_v[:, cols])
        y_copy(s).wait_recv()
        mixed = mixed + y_in[:, cols].astype(F32)
        upd_v[:, cols] = (x_v[:, cols].astype(F32) + mod_v[2:3, cols] * mixed).astype(BF16)
        out_copy(s).start()
        return carry

    lax.fori_loop(0, steps, finish, 0)

    for c in range(CHUNKS):
        for n in range(2):
            p1_copy(n, c).wait_send()
            forward_copy(n, c).wait_send()
            r_copy(n, c).wait_send()
            t_copy(n, c).wait_send()
        part_copy(c).wait_send()
    for s in range(steps):
        y_copy(s).wait_send()
        out_copy(s).wait()
    for step in range(2):
        at = pl.ds(pl.multiple_of(lax.rem(h + step, 2) * rows, rows), rows)
        pltpu.make_async_copy(fresh_v.at[:, at, :], fresh_h.at[:, at, :], fresh_sem.at[step]).wait()


def on_device(
    video_tokens, modulation, project_weight, output_weight, norm_gains,
    text_cache, text_count, video_keep, patch_order, stale_cache,
):
    rows, width = video_tokens.shape
    patch, local = stale_cache.shape[1:]
    hd = norm_gains.shape[1]
    heads = local // hd
    text_rows = text_cache.shape[1]
    half = local // 2
    sub = rows // CHUNKS
    key_rows = 3 * patch + text_rows
    keep = video_keep.reshape(-1, hd)
    y_steps = 3
    anywhere = pl.BlockSpec(memory_space=pl.ANY)
    scalars = pl.BlockSpec(memory_space=pltpu.SMEM)
    dma = pltpu.SemaphoreType.DMA
    vmem = pltpu.VMEM
    return pl.pallas_call(
        kernel,
        out_shape=(
            jax.ShapeDtypeStruct((rows, width), BF16),
            jax.ShapeDtypeStruct((2, patch, local), BF16),
        ),
        in_specs=[scalars, scalars] + [anywhere] * 8,
        out_specs=(anywhere, anywhere),
        scratch_shapes=[
            vmem((rows, width), BF16),
            vmem(modulation.shape, F32),
            vmem(project_weight.shape, BF16),
            vmem(output_weight.shape, BF16),
            vmem(norm_gains.shape, F32),
            vmem(text_cache.shape, BF16),
            vmem(keep.shape, jnp.int32),
            vmem(stale_cache.shape, BF16),
            vmem((patch, width), BF16),
            vmem((2, rows, width), BF16),
            vmem((CHUNKS, 4 * sub, width), BF16),
            vmem((2, patch, local), BF16),
            vmem((patch, local), BF16),
            vmem((key_rows, local), BF16),
            vmem((key_rows, local), BF16),
            vmem((2, key_rows, hd), BF16),
            vmem((patch, half), BF16),
            vmem((patch, half), BF16),
            vmem((4 * sub, half), BF16),
            vmem((heads, patch, 2 * hd), F32),
            vmem((2, CHUNKS, 2 * sub, half), BF16),
            vmem((2, CHUNKS, 2 * sub, half), BF16),
            vmem((2, CHUNKS, 8, 2 * sub), F32),
            vmem((2, CHUNKS, 8, 2 * sub), F32),
            vmem((patch, local), BF16),
            vmem((rows, width), BF16),
            vmem((rows, width), BF16),
            vmem((rows, width), BF16),
            dma((8,)),
            dma((CHUNKS,)),
            dma((CHUNKS,)),
            dma((2, CHUNKS)),
            dma((2, CHUNKS)),
            dma((2, CHUNKS)),
            dma((2, CHUNKS)),
            dma((2, CHUNKS)),
            dma((2, CHUNKS)),
            dma((2, CHUNKS)),
            dma((2, CHUNKS)),
            dma((y_steps,)),
            dma((y_steps,)),
            dma((y_steps,)),
            dma((2,)),
        ],
        compiler_params=pltpu.CompilerParams(
            collective_id=0, has_side_effects=True, vmem_limit_bytes=60 * 1024 * 1024
        ),
        name="patch_attention",
    )(
        patch_order, text_count, video_tokens, modulation, project_weight, output_weight,
        norm_gains, text_cache, keep, stale_cache,
    )


def solution(mesh):
    placed = (
        P(("groups", "section", "head"), None),
        P("groups", None),
        P(None, None, "head"),
        P("head", None),
        P(),
        P(None, "groups", "head"),
        P("groups"),
        P("groups"),
        P("groups"),
        P(None, ("groups", "section"), "head"),
    )
    return jax.shard_map(
        on_device,
        mesh=mesh,
        in_specs=placed,
        out_specs=(P(("groups", "section", "head"), None), P(None, ("groups", "section"), "head")),
        check_vma=False,
    )
```

```python
import functools
import math

import jax
import jax.numpy as jnp
from jax import lax
from jax.experimental import pallas as pl
from jax.experimental.pallas import tpu as pltpu
from jax.sharding import PartitionSpec as P

epsilon = 1e-06
CHUNKS = 2
F32 = jnp.float32
BF16 = jnp.bfloat16
MESH = pl.DeviceIdType.MESH
NT = (((1,), (1,)), ((), ()))


def matmul(a, b):
    return jnp.dot(a, b, preferred_element_type=F32)


def head_norm(values, gain):
    square = jnp.mean(values * values, axis=-1, keepdims=True)
    return values * lax.rsqrt(square + epsilon) * gain


def kernel(
    order_s, count_s, x_h, mod_h, w_h, wo_h, gains_h, text_h, keep_h, stale_h,
    updated_h, fresh_h,
    x_v, mod_v, w_v, wo_v, gains_v, text_v, keep_v, stale_v,
    normed, message, arrived, extra, raw, q_own, kbuf, vbuf, mbuf, acc, attended, y_sum, y_out, y_in, fresh_v, updated_v,
    load_sem, part_send, part_recv, p1_send, p1_recv, f_send, f_recv, e_send, e_recv, y_send, y_recv, out_sem,
    left_ready, partner_ready,
):
    rows, width = x_v.shape
    patch, local = stale_v.shape[1], stale_v.shape[2]
    text_rows = text_v.shape[1]
    hd = gains_v.shape[1]
    heads = local // hd
    half_heads = heads // 2
    half = half_heads * hd
    sub = rows // CHUNKS
    wide = 2 * hd
    sections = lax.axis_size("section")
    place = lax.axis_index("section")
    h = lax.axis_index("head")
    nbr_place = (jnp.maximum(place - 1, 0), jnp.minimum(place + 1, sections - 1))
    nbr_of = ({"section": nbr_place[0]}, {"section": nbr_place[1]})
    partner = {"head": 1 - h}
    exists = (place > 0, place < sections - 1)
    inner = (place > 0) & (place < sections - 1)

    def for_neighbour(n, work):
        pl.when(exists[n])(work)

    barrier = pltpu.get_barrier_semaphore()
    for_neighbour(0, lambda: pl.semaphore_signal(barrier, inc=1, device_id=nbr_of[0], device_id_type=MESH))

    @pl.when(h == 1)
    def _():
        pl.semaphore_signal(barrier, inc=1, device_id=partner, device_id_type=MESH)

    sources = [
        (x_h, x_v), (mod_h, mod_v), (stale_h, stale_v), (gains_h, gains_v), (keep_h, keep_v),
        (w_h.at[1], w_v.at[1]), (w_h.at[2], w_v.at[2]), (w_h.at[0], w_v.at[0]), (text_h, text_v), (wo_h, wo_v),
    ]
    loads = [pltpu.make_async_copy(src, dst, load_sem.at[i]) for i, (src, dst) in enumerate(sources)]
    for load in loads:
        load.start()

    own_slot = order_s[place]
    slot = (order_s[nbr_place[0]], order_s[nbr_place[1]])
    one = jnp.int32(1)
    zero = jnp.int32(0)
    is_b = [jnp.where(slot[n] < own_slot, one, zero) for n in range(2)]
    is_a = [jnp.where(own_slot < slot[n], one, zero) for n in range(2)]

    def full(flag, shape):
        return jnp.full(shape, flag, jnp.int32) > 0

    base = pl.multiple_of(h * rows, rows)

    def area(n, core):
        return pl.ds(pl.multiple_of((2 * n + core) * sub, sub), sub)

    def p1_copy(n, c, side):
        at = pl.ds(pl.multiple_of(c * sub, sub), sub)
        return pltpu.make_async_remote_copy(
            src_ref=message.at[n, at, :],
            dst_ref=arrived.at[c, area(side, h), :],
            send_sem=p1_send.at[n, c],
            recv_sem=p1_recv.at[side, c],
            device_id=nbr_of[n],
            device_id_type=MESH,
        )

    def extra_copy(n, kind, i, side):
        cols = slice(i * hd, (i + 1) * hd)
        return pltpu.make_async_remote_copy(
            src_ref=stale_v.at[kind, :, cols],
            dst_ref=extra.at[side, kind, :, cols],
            send_sem=e_send.at[n, kind, i],
            recv_sem=e_recv.at[side, kind, i],
            device_id=nbr_of[n],
            device_id_type=MESH,
        )

    def part_copy(c, core):
        at = pl.ds(pl.multiple_of(core * rows + c * sub, sub), sub)
        return pltpu.make_async_remote_copy(
            src_ref=normed.at[at, :],
            dst_ref=normed.at[at, :],
            send_sem=part_send.at[c],
            recv_sem=part_recv.at[c],
            device_id=partner,
            device_id_type=MESH,
        )

    def forward_copy(n, c, core):
        return pltpu.make_async_remote_copy(
            src_ref=arrived.at[c, area(n, core), :],
            dst_ref=arrived.at[c, area(n, core), :],
            send_sem=f_send.at[n, c],
            recv_sem=f_recv.at[n, c],
            device_id=partner,
            device_id_type=MESH,
        )

    extras = [(kind, i) for i in range(half_heads) for kind in range(2)]

    def send_extras(n):
        for kind, i in extras:
            extra_copy(n, kind, i, 1 - n).start()

    def meet_left():
        pl.semaphore_wait(left_ready, 1)
        for c in range(CHUNKS):
            p1_copy(0, c, 1).start()

    def swap_parts():
        for c in range(CHUNKS):
            part_copy(c, h).start()

    def meet_right():
        needed = jnp.where(place < sections - 1, one, zero) + jnp.where(h == 0, one, zero)
        pl.when(needed > 0)(lambda: pl.semaphore_wait(barrier, needed))
        for_neighbour(1, lambda: pl.semaphore_signal(left_ready, inc=1, device_id=nbr_of[1], device_id_type=MESH))

        @pl.when(h == 0)
        def _():
            pl.semaphore_signal(partner_ready, inc=1, device_id=partner, device_id_type=MESH)

    def meet_partner():
        pl.semaphore_wait(partner_ready, 1)
        swap_parts()

    loads[0].wait()
    loads[1].wait()
    scale = 1.0 + mod_v[1:2, :]
    shift = mod_v[0:1, :]
    piece = sub // 2
    for c in range(CHUNKS):
        for p in range(2):
            at = slice(c * sub + p * piece, c * sub + (p + 1) * piece)
            hidden = x_v[at, :].astype(F32)
            center = jnp.mean(hidden, axis=-1, keepdims=True)
            shifted = hidden - center
            spread = jnp.mean(shifted * shifted, axis=-1, keepdims=True)
            tokens = (shifted * lax.rsqrt(spread + epsilon) * scale + shift).astype(BF16)
            normed[pl.ds(pl.multiple_of(base + c * sub + p * piece, piece), piece), :] = tokens
            if c == 0 and p == 0:
                meet_right()
                loads[2].wait()
            other = slice(rows + c * sub + p * piece, rows + c * sub + (p + 1) * piece)
            packed = jnp.concatenate(
                [stale_v[0, at, half:], stale_v[0, other, half:], stale_v[1, at, half:], stale_v[1, other, half:]],
                axis=1,
            )
            for n in range(2):
                message[n, at, :] = jnp.where(full(is_a[n], tokens.shape), tokens, packed)
        for_neighbour(1, lambda c=c: p1_copy(1, c, 0).start())

    waits = (place == 1) & (h == 0)
    pl.when((place > 0) & jnp.logical_not(waits))(meet_left)
    pl.when(h == 0)(swap_parts)
    pl.when((h == 1) & (place > 0))(meet_partner)

    for i in (3, 4):
        loads[i].wait()
    near = patch + text_rows

    def keep_column(index, part):
        row = keep_v[pl.ds(index * (patch // hd) + part, 1), :]
        return jnp.transpose(jnp.broadcast_to(row.astype(F32), (hd, hd))).astype(BF16)

    for part in range(patch // hd):
        low = part * hd
        mbuf[low : low + hd, :] = keep_column(place, part)
        for n in range(2):
            mbuf[near + n * patch + low : near + n * patch + low + hd, :] = keep_column(nbr_place[n], part)
    live = lax.broadcasted_iota(jnp.int32, (text_rows, hd), 0) < count_s[0]
    mbuf[patch:near, :] = jnp.where(live, 1.0, 0.0).astype(BF16)

    q_gain = gains_v[0:1, :] * (math.log2(math.e) * hd**-0.5)
    k_gain = gains_v[1:2, :]
    t_gain = gains_v[2:3, :]

    def own(at, index, beside):
        for i in range(local // wide):
            block = slice(i * wide, (i + 1) * wide)
            result = matmul(normed[at, :], w_v[index, :, block])
            if index > 0:
                result = result.astype(BF16)
                fresh_v[index - 1, at, block] = result
            for j in range(2):
                lanes = slice(j * hd, (j + 1) * hd)
                cols = slice(i * wide + j * hd, i * wide + (j + 1) * hd)
                if index == 0:
                    q_own[at, cols] = head_norm(result[:, lanes], q_gain).astype(BF16)
                if index == 1:
                    kbuf[at, cols] = head_norm(result[:, lanes].astype(F32), k_gain).astype(BF16)
                if index == 2:
                    vbuf[at, cols] = result[:, lanes] * mbuf[at, :]
                if beside:
                    kbuf[patch:near, cols] = head_norm(text_v[0, :, cols].astype(F32), t_gain).astype(BF16)
                    vbuf[patch:near, cols] = text_v[1, :, cols] * mbuf[patch:near, :]

    for step in range(2):
        side = h if step == 0 else 1 - h
        at = pl.ds(pl.multiple_of(side * rows, rows), rows)
        if step == 1:
            for_neighbour(1, lambda: send_extras(1))
            pl.when((h == 1) & (place == 0))(meet_partner)
            pl.when((place > 0) & jnp.logical_not(waits))(lambda: send_extras(0))
            for c in range(CHUNKS):
                part_copy(c, 1 - h).wait_recv()
        for index in (1, 2, 0):
            if step == 0:
                loads[{1: 5, 2: 6, 0: 7}[index]].wait()
            if step == 1 and index == 1:
                loads[8].wait()
            own(at, index, step == 1 and index == 1)
        pltpu.make_async_copy(fresh_v.at[:, at, :], fresh_h.at[:, at, :], out_sem.at[step]).start()

    def take(n, c):
        p1_copy(n, c, n).wait_recv()
        forward_copy(n, c, h).start()

    def scores(query, key):
        return lax.dot_general(query, key, NT, preferred_element_type=F32)

    def attend(at, i):
        cols = slice(i * hd, (i + 1) * hd)
        weight = jnp.exp2(scores(q_own[:, cols], kbuf[at, cols])).astype(BF16)
        return matmul(weight, jnp.concatenate([vbuf[at, cols], mbuf[at, :]], axis=1))

    for i in range(heads):
        acc[i] = attend(slice(0, near), i)

    def job(n, c):
        forward_copy(n, c, 1 - h).wait_recv()
        tokens = arrived.at[c, pl.ds(2 * n * sub, 2 * sub), :]
        pick = full(is_b[n], (sub, hd))
        for i in reversed(range(local // wide)):
            block = slice(i * wide, (i + 1) * wide)
            for kind in range(2):
                result = matmul(tokens[...], w_v[1 + kind, :, block]).astype(BF16)
                for j in range(2):
                    head = 2 * i + j
                    cols = slice(head * hd, (head + 1) * hd)
                    for core in range(2):
                        part = result[core * sub : (core + 1) * sub, j * hd : (j + 1) * hd]
                        row = pl.multiple_of(core * rows + c * sub, sub)
                        if head < half_heads:
                            raw[n, kind, pl.ds(row, sub), cols] = part
                            continue
                        low = (2 * kind + core) * half + (head - half_heads) * hd
                        part = jnp.where(pick, part, arrived[c, area(n, h), low : low + hd])
                        to = pl.ds(pl.multiple_of(near + n * patch + row, sub), sub)
                        if kind == 0:
                            kbuf[to, cols] = head_norm(part.astype(F32), k_gain).astype(BF16)
                        else:
                            vbuf[to, cols] = part * mbuf[to, :]

    def take_left(chunks):
        for c in chunks:
            take(0, c)

    ready = (place > 0) & jnp.logical_not(waits)
    for c in range(CHUNKS):
        for_neighbour(1, lambda: take(1, c))
        pl.when(ready)(lambda: take(0, c))
        for_neighbour(1, lambda: job(1, c))
        if c == 0:

            @pl.when(waits)
            def _():
                meet_left()
                send_extras(0)

    pl.when(waits)(lambda: take_left(range(CHUNKS)))

    @pl.when(exists[0])
    def _():
        for c in range(CHUNKS):
            job(0, c)

    def finish_head(at, i):
        cols = slice(i * hd, (i + 1) * hd)
        both = acc[i] + attend(at, i)
        attended[:, cols] = (both[:, :hd] / both[:, hd:]).astype(BF16)

    def finish_heads(which):
        @pl.when(inner)
        def _():
            for i in which:
                finish_head(slice(near, near + 2 * patch), i)

        @pl.when(jnp.logical_not(inner))
        def _():
            at = pl.ds(pl.multiple_of(near + jnp.where(place > 0, 0, patch), 2 * sub), patch)
            for i in which:
                finish_head(at, i)

    def take_extra(n, i):
        for kind in range(2):
            extra_copy(n, kind, i, n).wait_recv()
        cols = slice(i * hd, (i + 1) * hd)
        pick = full(is_b[n], (patch, hd))
        to = slice(near + n * patch, near + (n + 1) * patch)
        k_part = jnp.where(pick, raw[n, 0, :, cols], extra[n, 0, :, cols])
        v_part = jnp.where(pick, raw[n, 1, :, cols], extra[n, 1, :, cols])
        kbuf[to, cols] = head_norm(k_part.astype(F32), k_gain).astype(BF16)
        vbuf[to, cols] = v_part * mbuf[to, :]

    def extra_head(i):
        for n in (1, 0):
            for_neighbour(n, lambda n=n: take_extra(n, i))
        finish_heads([i])

    steps = y_send.shape[0]
    span = width // steps

    def partial_sum(pair, first):
        lanes = slice(pair * wide, (pair + 1) * wide)
        for s in range(steps):
            cols = slice(s * span, (s + 1) * span)
            part = matmul(attended[:, lanes], wo_v[lanes, cols])
            y_sum[:, cols] = part if first else y_sum[:, cols] + part

    finish_heads(range(half_heads, heads))
    loads[9].wait()
    last = (half_heads - 1) // 2
    late_pairs = [pair for pair in range(heads // 2) if 2 * pair + 1 < half_heads]
    early_pairs = [pair for pair in range(heads // 2) if 2 * pair >= half_heads]
    for k, pair in enumerate(early_pairs):
        partial_sum(pair, k == 0)
    for i in range(half_heads - 1):
        extra_head(i)
    for pair in late_pairs:
        partial_sum(pair, False)
    extra_head(half_heads - 1)

    lanes = slice(last * wide, (last + 1) * wide)
    other = pl.ds(pl.multiple_of((1 - h) * rows, rows), rows)
    mine = pl.ds(base, rows)

    def y_copy(s):
        cols = slice(s * span, (s + 1) * span)
        return pltpu.make_async_remote_copy(
            src_ref=y_out.at[:, cols],
            dst_ref=y_in.at[:, cols],
            send_sem=y_send.at[s],
            recv_sem=y_recv.at[s],
            device_id=partner,
            device_id_type=MESH,
        )

    for s in range(steps):
        cols = slice(s * span, (s + 1) * span)
        y_out[:, cols] = (y_sum[other, cols] + matmul(attended[other, lanes], wo_v[lanes, cols])).astype(BF16)
        y_copy(s).start()
    for s in range(steps):
        cols = slice(s * span, (s + 1) * span)
        y_sum[mine, cols] += matmul(attended[mine, lanes], wo_v[lanes, cols])
    for s in range(steps):
        cols = slice(s * span, (s + 1) * span)
        y_copy(s).wait_recv()
        mixed = y_sum[mine, cols] + y_in[:, cols].astype(F32)
        updated_v[:, cols] = (x_v[:, cols].astype(F32) + mod_v[2:3, cols] * mixed).astype(BF16)
        pltpu.make_async_copy(updated_v.at[:, cols], updated_h.at[:, cols], out_sem.at[2 + s]).start()

    def sent_to(n):
        for c in range(CHUNKS):
            p1_copy(n, c, 1 - n).wait_send()
            forward_copy(n, c, h).wait_send()
        for kind, i in extras:
            extra_copy(n, kind, i, 1 - n).wait_send()

    for n in range(2):
        for_neighbour(n, lambda n=n: sent_to(n))
    for c in range(CHUNKS):
        part_copy(c, h).wait_send()
    for s in range(steps):
        y_copy(s).wait_send()
        cols = slice(s * span, (s + 1) * span)
        pltpu.make_async_copy(updated_v.at[:, cols], updated_h.at[:, cols], out_sem.at[2 + s]).wait()
    for step in range(2):
        at = pl.ds(pl.multiple_of(jnp.where(step == 0, h, 1 - h) * rows, rows), rows)
        pltpu.make_async_copy(fresh_v.at[:, at, :], fresh_h.at[:, at, :], out_sem.at[step]).wait()


def on_device(
    video_tokens, modulation, project_weight, output_weight, norm_gains,
    text_cache, text_count, video_keep, patch_order, stale_cache,
):
    rows, width = video_tokens.shape
    patch, local = stale_cache.shape[1:]
    hd = norm_gains.shape[1]
    heads = local // hd
    text_rows = text_cache.shape[1]
    half = local // 2
    sub = rows // CHUNKS
    key_rows = 3 * patch + text_rows
    keep = video_keep.reshape(-1, hd)
    y_steps = 3
    anywhere = pl.BlockSpec(memory_space=pl.ANY)
    scalars = pl.BlockSpec(memory_space=pltpu.SMEM)
    dma = pltpu.SemaphoreType.DMA
    vmem = pltpu.VMEM
    return pl.pallas_call(
        kernel,
        out_shape=(
            jax.ShapeDtypeStruct((rows, width), BF16),
            jax.ShapeDtypeStruct((2, patch, local), BF16),
        ),
        in_specs=[scalars, scalars] + [anywhere] * 8,
        out_specs=(anywhere, anywhere),
        scratch_shapes=[
            vmem((rows, width), BF16),
            vmem(modulation.shape, F32),
            vmem(project_weight.shape, BF16),
            vmem(output_weight.shape, BF16),
            vmem(norm_gains.shape, F32),
            vmem(text_cache.shape, BF16),
            vmem(keep.shape, jnp.int32),
            vmem(stale_cache.shape, BF16),
            vmem((patch, width), BF16),
            vmem((2, rows, width), BF16),
            vmem((CHUNKS, 4 * sub, width), BF16),
            vmem((2, 2, patch, half), BF16),
            vmem((2, 2, patch, half), BF16),
            vmem((patch, local), BF16),
            vmem((key_rows, local), BF16),
            vmem((key_rows, local), BF16),
            vmem((key_rows, hd), BF16),
            vmem((heads, patch, 2 * hd), F32),
            vmem((patch, local), BF16),
            vmem((patch, width), F32),
            vmem((rows, width), BF16),
            vmem((rows, width), BF16),
            vmem((2, patch, local), BF16),
            vmem((rows, width), BF16),
            dma((10,)),
            dma((CHUNKS,)),
            dma((CHUNKS,)),
            dma((2, CHUNKS)),
            dma((2, CHUNKS)),
            dma((2, CHUNKS)),
            dma((2, CHUNKS)),
            dma((2, 2, heads // 2)),
            dma((2, 2, heads // 2)),
            dma((y_steps,)),
            dma((y_steps,)),
            dma((2 + y_steps,)),
            pltpu.SemaphoreType.REGULAR,
            pltpu.SemaphoreType.REGULAR,
        ],
        compiler_params=pltpu.CompilerParams(
            collective_id=0, has_side_effects=True, vmem_limit_bytes=60 * 1024 * 1024
        ),
        name="patch_attention",
    )(
        patch_order, text_count, video_tokens, modulation, project_weight, output_weight,
        norm_gains, text_cache, keep, stale_cache,
    )


def solution(mesh):
    placed = (
        P(("groups", "section", "head"), None),
        P("groups", None),
        P(None, None, "head"),
        P("head", None),
        P(),
        P(None, "groups", "head"),
        P("groups"),
        P("groups"),
        P("groups"),
        P(None, ("groups", "section"), "head"),
    )
    return jax.shard_map(
        on_device,
        mesh=mesh,
        in_specs=placed,
        out_specs=(P(("groups", "section", "head"), None), P(None, ("groups", "section"), "head")),
        check_vma=False,
    )
```

```python
import functools
import math

import jax
import jax.numpy as jnp
from jax import lax
from jax.experimental import pallas as pl
from jax.experimental.pallas import tpu as pltpu
from jax.sharding import PartitionSpec as P

epsilon = 1e-06
CHUNKS = 2
F32 = jnp.float32
BF16 = jnp.bfloat16
MESH = pl.DeviceIdType.MESH
NT = (((1,), (1,)), ((), ()))


def matmul(a, b):
    return jnp.dot(a, b, preferred_element_type=F32)


def head_norm(values, gain):
    square = jnp.mean(values * values, axis=-1, keepdims=True)
    return values * lax.rsqrt(square + epsilon) * gain


def kernel(
    order_h, count_h, x_h, mod_h, w_h, wo_h, gains_h, text_h, keep_h, stale_h,
    updated_h, fresh_h,
    x_v, mod_v, w_v, wo_v, gains_v, text_v, keep_v, stale_v,
    normed, message, arrived, extra, raw, q_own, kbuf, vbuf, mbuf, acc, attended, y_sum, y_out, y_in, fresh_v, updated_v, order_s, count_s,
    load_sem, part_send, part_recv, p1_send, p1_recv, f_send, f_recv, e_send, e_recv, y_send, y_recv, out_sem,
    left_ready, partner_ready,
):
    rows, width = x_v.shape
    patch, local = stale_v.shape[1], stale_v.shape[2]
    text_rows = text_v.shape[1]
    hd = gains_v.shape[1]
    heads = local // hd
    half_heads = heads // 2
    half = half_heads * hd
    sub = rows // CHUNKS
    wide = 2 * hd
    sections = lax.axis_size("section")
    place = lax.axis_index("section")
    h = lax.axis_index("head")
    nbr_place = (jnp.maximum(place - 1, 0), jnp.minimum(place + 1, sections - 1))
    nbr_of = ({"section": nbr_place[0]}, {"section": nbr_place[1]})
    partner = {"head": 1 - h}
    exists = (place > 0, place < sections - 1)
    inner = (place > 0) & (place < sections - 1)

    def for_neighbour(n, work):
        pl.when(exists[n])(work)

    barrier = pltpu.get_barrier_semaphore()
    for_neighbour(0, lambda: pl.semaphore_signal(barrier, inc=1, device_id=nbr_of[0], device_id_type=MESH))

    @pl.when(h == 1)
    def _():
        pl.semaphore_signal(barrier, inc=1, device_id=partner, device_id_type=MESH)

    sources = [
        (order_h, order_s), (mod_h, mod_v), (stale_h, stale_v), (gains_h, gains_v), (keep_h, keep_v),
        (w_h.at[1], w_v.at[1]), (w_h.at[2], w_v.at[2]), (w_h.at[0], w_v.at[0]), (text_h, text_v), (wo_h, wo_v), (count_h, count_s),
    ]
    piece = sub // 2
    sources += [(x_h.at[pl.ds(i * piece, piece), :], x_v.at[pl.ds(i * piece, piece), :]) for i in range(2 * CHUNKS)]
    first_piece = len(sources) - 2 * CHUNKS
    loads = [pltpu.make_async_copy(src, dst, load_sem.at[i]) for i, (src, dst) in enumerate(sources)]
    for i in (*range(first_piece, len(loads)), *range(first_piece)):
        loads[i].start()

    one = jnp.int32(1)
    zero = jnp.int32(0)

    def full(flag, shape):
        return jnp.full(shape, flag, jnp.int32) > 0

    base = pl.multiple_of(h * rows, rows)

    def area(n, core):
        return pl.ds(pl.multiple_of((2 * n + core) * sub, sub), sub)

    def p1_copy(n, c, side):
        at = pl.ds(pl.multiple_of(c * sub, sub), sub)
        return pltpu.make_async_remote_copy(
            src_ref=message.at[n, at, :],
            dst_ref=arrived.at[c, area(side, h), :],
            send_sem=p1_send.at[n, c],
            recv_sem=p1_recv.at[side, c],
            device_id=nbr_of[n],
            device_id_type=MESH,
        )

    def extra_copy(n, kind, i, side):
        cols = slice(i * hd, (i + 1) * hd)
        return pltpu.make_async_remote_copy(
            src_ref=stale_v.at[kind, :, cols],
            dst_ref=extra.at[side, kind, :, cols],
            send_sem=e_send.at[n, kind, i],
            recv_sem=e_recv.at[side, kind, i],
            device_id=nbr_of[n],
            device_id_type=MESH,
        )

    def part_copy(c, core):
        at = pl.ds(pl.multiple_of(core * rows + c * sub, sub), sub)
        return pltpu.make_async_remote_copy(
            src_ref=normed.at[at, :],
            dst_ref=normed.at[at, :],
            send_sem=part_send.at[c],
            recv_sem=part_recv.at[c],
            device_id=partner,
            device_id_type=MESH,
        )

    def forward_copy(n, c, core):
        return pltpu.make_async_remote_copy(
            src_ref=arrived.at[c, area(n, core), :],
            dst_ref=arrived.at[c, area(n, core), :],
            send_sem=f_send.at[n, c],
            recv_sem=f_recv.at[n, c],
            device_id=partner,
            device_id_type=MESH,
        )

    extras = [(kind, i) for i in range(half_heads) for kind in range(2)]

    def send_extras(n):
        for kind, i in extras:
            extra_copy(n, kind, i, 1 - n).start()

    def meet_left():
        pl.semaphore_wait(left_ready, 1)
        for c in range(CHUNKS):
            p1_copy(0, c, 1).start()

    def swap_parts():
        for c in range(CHUNKS):
            part_copy(c, h).start()

    def meet_right():
        needed = jnp.where(place < sections - 1, one, zero) + jnp.where(h == 0, one, zero)
        pl.when(needed > 0)(lambda: pl.semaphore_wait(barrier, needed))
        for_neighbour(1, lambda: pl.semaphore_signal(left_ready, inc=1, device_id=nbr_of[1], device_id_type=MESH))

        @pl.when(h == 0)
        def _():
            pl.semaphore_signal(partner_ready, inc=1, device_id=partner, device_id_type=MESH)

    def meet_partner():
        pl.semaphore_wait(partner_ready, 1)
        swap_parts()

    loads[1].wait()
    loads[0].wait()
    own_slot = order_s[place]
    slot = (order_s[nbr_place[0]], order_s[nbr_place[1]])
    is_b = [jnp.where(slot[n] < own_slot, one, zero) for n in range(2)]
    is_a = [jnp.where(own_slot < slot[n], one, zero) for n in range(2)]
    scale = 1.0 + mod_v[1:2, :]
    shift = mod_v[0:1, :]
    for c in range(CHUNKS):
        for p in range(2):
            at = slice(c * sub + p * piece, c * sub + (p + 1) * piece)
            loads[first_piece + 2 * c + p].wait()
            hidden = x_v[at, :].astype(F32)
            center = jnp.mean(hidden, axis=-1, keepdims=True)
            shifted = hidden - center
            spread = jnp.mean(shifted * shifted, axis=-1, keepdims=True)
            tokens = (shifted * lax.rsqrt(spread + epsilon) * scale + shift).astype(BF16)
            normed[pl.ds(pl.multiple_of(base + c * sub + p * piece, piece), piece), :] = tokens
            if c == 0 and p == 0:
                meet_right()
                loads[2].wait()
            other = slice(rows + c * sub + p * piece, rows + c * sub + (p + 1) * piece)
            packed = jnp.concatenate(
                [stale_v[0, at, half:], stale_v[0, other, half:], stale_v[1, at, half:], stale_v[1, other, half:]],
                axis=1,
            )
            for n in range(2):
                message[n, at, :] = jnp.where(full(is_a[n], tokens.shape), tokens, packed)
        for_neighbour(1, lambda c=c: p1_copy(1, c, 0).start())

    waits = (place == 1) & (h == 0)
    pl.when((place > 0) & jnp.logical_not(waits))(meet_left)
    pl.when(h == 0)(swap_parts)
    pl.when((h == 1) & (place > 0))(meet_partner)

    for i in (3, 4, 10):
        loads[i].wait()
    near = patch + text_rows

    def keep_column(index, part):
        row = keep_v[pl.ds(index * (patch // hd) + part, 1), :]
        return jnp.transpose(jnp.broadcast_to(row.astype(F32), (hd, hd))).astype(BF16)

    for part in range(patch // hd):
        low = part * hd
        mbuf[low : low + hd, :] = keep_column(place, part)
        for n in range(2):
            mbuf[near + n * patch + low : near + n * patch + low + hd, :] = keep_column(nbr_place[n], part)
    live = lax.broadcasted_iota(jnp.int32, (text_rows, hd), 0) < count_s[0]
    mbuf[patch:near, :] = jnp.where(live, 1.0, 0.0).astype(BF16)

    q_gain = gains_v[0:1, :] * (math.log2(math.e) * hd**-0.5)
    k_gain = gains_v[1:2, :]
    t_gain = gains_v[2:3, :]

    def own(at, index, beside):
        for i in range(local // wide):
            block = slice(i * wide, (i + 1) * wide)
            result = matmul(normed[at, :], w_v[index, :, block])
            if index > 0:
                result = result.astype(BF16)
                fresh_v[index - 1, at, block] = result
            for j in range(2):
                lanes = slice(j * hd, (j + 1) * hd)
                cols = slice(i * wide + j * hd, i * wide + (j + 1) * hd)
                if index == 0:
                    q_own[at, cols] = head_norm(result[:, lanes], q_gain).astype(BF16)
                if index == 1:
                    kbuf[at, cols] = head_norm(result[:, lanes].astype(F32), k_gain).astype(BF16)
                if index == 2:
                    vbuf[at, cols] = result[:, lanes] * mbuf[at, :]
                if beside:
                    kbuf[patch:near, cols] = head_norm(text_v[0, :, cols].astype(F32), t_gain).astype(BF16)
                    vbuf[patch:near, cols] = text_v[1, :, cols] * mbuf[patch:near, :]

    for step in range(2):
        side = h if step == 0 else 1 - h
        at = pl.ds(pl.multiple_of(side * rows, rows), rows)
        if step == 1:
            for_neighbour(1, lambda: send_extras(1))
            pl.when((h == 1) & (place == 0))(meet_partner)
            pl.when((place > 0) & jnp.logical_not(waits))(lambda: send_extras(0))
            for c in range(CHUNKS):
                part_copy(c, 1 - h).wait_recv()
        for index in (1, 2, 0):
            if step == 0:
                loads[{1: 5, 2: 6, 0: 7}[index]].wait()
            if step == 1 and index == 1:
                loads[8].wait()
            own(at, index, step == 1 and index == 1)
        pltpu.make_async_copy(fresh_v.at[:, at, :], fresh_h.at[:, at, :], out_sem.at[step]).start()

    def take(n, c):
        p1_copy(n, c, n).wait_recv()
        forward_copy(n, c, h).start()

    def scores(query, key):
        return lax.dot_general(query, key, NT, preferred_element_type=F32)

    def attend(at, i):
        cols = slice(i * hd, (i + 1) * hd)
        weight = jnp.exp2(scores(q_own[:, cols], kbuf[at, cols])).astype(BF16)
        return matmul(weight, jnp.concatenate([vbuf[at, cols], mbuf[at, :]], axis=1))

    pl.when(place == 0)(lambda: take(1, 0))
    for i in range(heads):
        acc[i] = attend(slice(0, near), i)

    def job(n, c):
        forward_copy(n, c, 1 - h).wait_recv()
        tokens = arrived.at[c, pl.ds(2 * n * sub, 2 * sub), :]
        pick = full(is_b[n], (sub, hd))
        for i in reversed(range(local // wide)):
            block = slice(i * wide, (i + 1) * wide)
            for kind in range(2):
                result = matmul(tokens[...], w_v[1 + kind, :, block]).astype(BF16)
                for j in range(2):
                    head = 2 * i + j
                    cols = slice(head * hd, (head + 1) * hd)
                    for core in range(2):
                        part = result[core * sub : (core + 1) * sub, j * hd : (j + 1) * hd]
                        row = pl.multiple_of(core * rows + c * sub, sub)
                        if head < half_heads:
                            raw[n, kind, pl.ds(row, sub), cols] = part
                            continue
                        low = (2 * kind + core) * half + (head - half_heads) * hd
                        part = jnp.where(pick, part, arrived[c, area(n, h), low : low + hd])
                        to = pl.ds(pl.multiple_of(near + n * patch + row, sub), sub)
                        if kind == 0:
                            kbuf[to, cols] = head_norm(part.astype(F32), k_gain).astype(BF16)
                        else:
                            vbuf[to, cols] = part * mbuf[to, :]

    def jobs(t, carry):
        delay = jnp.where(place == 1, CHUNKS, 0)
        has_right = exists[1] & (t < CHUNKS)
        has_left = exists[0] & (t >= delay) & (t < delay + CHUNKS)

        @pl.when(waits & (t == 1))
        def _():
            meet_left()
            send_extras(0)

        pl.when(has_right & (place > 0))(lambda: take(1, t))
        pl.when(has_left)(lambda: take(0, t - delay))

        @pl.when((place == 0) & (t == 0))
        def _():
            for c in range(1, CHUNKS):
                take(1, c)

        pl.when(has_right)(lambda: job(1, t))
        pl.when(has_left)(lambda: job(0, t - delay))
        return carry

    lax.fori_loop(0, 2 * CHUNKS, jobs, 0)

    def finish_head(at, i):
        cols = slice(i * hd, (i + 1) * hd)
        both = acc[i] + attend(at, i)
        attended[:, cols] = (both[:, :hd] / both[:, hd:]).astype(BF16)

    def finish_heads(which):
        @pl.when(inner)
        def _():
            for i in which:
                finish_head(slice(near, near + 2 * patch), i)

        @pl.when(jnp.logical_not(inner))
        def _():
            at = pl.ds(pl.multiple_of(near + jnp.where(place > 0, 0, patch), 2 * sub), patch)
            for i in which:
                finish_head(at, i)

    def take_extra(n, i):
        for kind in range(2):
            extra_copy(n, kind, i, n).wait_recv()
        cols = slice(i * hd, (i + 1) * hd)
        pick = full(is_b[n], (patch, hd))
        to = slice(near + n * patch, near + (n + 1) * patch)
        k_part = jnp.where(pick, raw[n, 0, :, cols], extra[n, 0, :, cols])
        v_part = jnp.where(pick, raw[n, 1, :, cols], extra[n, 1, :, cols])
        kbuf[to, cols] = head_norm(k_part.astype(F32), k_gain).astype(BF16)
        vbuf[to, cols] = v_part * mbuf[to, :]

    def extra_head(i):
        for n in (1, 0):
            for_neighbour(n, lambda n=n: take_extra(n, i))
        finish_heads([i])

    steps = y_send.shape[0]
    span = width // steps

    def partial_sum(pair, first):
        lanes = slice(pair * wide, (pair + 1) * wide)
        for s in range(steps):
            cols = slice(s * span, (s + 1) * span)
            part = matmul(attended[:, lanes], wo_v[lanes, cols])
            y_sum[:, cols] = part if first else y_sum[:, cols] + part

    finish_heads(range(half_heads, heads))
    loads[9].wait()
    last = (half_heads - 1) // 2
    late_pairs = [pair for pair in range(heads // 2) if 2 * pair + 1 < half_heads]
    early_pairs = [pair for pair in range(heads // 2) if 2 * pair >= half_heads]
    for k, pair in enumerate(early_pairs):
        partial_sum(pair, k == 0)
    for i in range(half_heads - 1):
        extra_head(i)
    for pair in late_pairs:
        partial_sum(pair, False)
    extra_head(half_heads - 1)

    lanes = slice(last * wide, (last + 1) * wide)
    other = pl.ds(pl.multiple_of((1 - h) * rows, rows), rows)
    mine = pl.ds(base, rows)

    def y_copy(s):
        cols = slice(s * span, (s + 1) * span)
        return pltpu.make_async_remote_copy(
            src_ref=y_out.at[:, cols],
            dst_ref=y_in.at[:, cols],
            send_sem=y_send.at[s],
            recv_sem=y_recv.at[s],
            device_id=partner,
            device_id_type=MESH,
        )

    for s in range(steps):
        cols = slice(s * span, (s + 1) * span)
        y_out[:, cols] = (y_sum[other, cols] + matmul(attended[other, lanes], wo_v[lanes, cols])).astype(BF16)
        y_copy(s).start()
    for s in range(steps):
        cols = slice(s * span, (s + 1) * span)
        y_sum[mine, cols] += matmul(attended[mine, lanes], wo_v[lanes, cols])
    for s in range(steps):
        cols = slice(s * span, (s + 1) * span)
        y_copy(s).wait_recv()
        mixed = y_sum[mine, cols] + y_in[:, cols].astype(F32)
        updated_v[:, cols] = (x_v[:, cols].astype(F32) + mod_v[2:3, cols] * mixed).astype(BF16)
        pltpu.make_async_copy(updated_v.at[:, cols], updated_h.at[:, cols], out_sem.at[2 + s]).start()

    def sent_to(n):
        for c in range(CHUNKS):
            p1_copy(n, c, 1 - n).wait_send()
            forward_copy(n, c, h).wait_send()
        for kind, i in extras:
            extra_copy(n, kind, i, 1 - n).wait_send()

    for n in range(2):
        for_neighbour(n, lambda n=n: sent_to(n))
    for c in range(CHUNKS):
        part_copy(c, h).wait_send()
    for s in range(steps):
        y_copy(s).wait_send()
        cols = slice(s * span, (s + 1) * span)
        pltpu.make_async_copy(updated_v.at[:, cols], updated_h.at[:, cols], out_sem.at[2 + s]).wait()
    for step in range(2):
        at = pl.ds(pl.multiple_of(jnp.where(step == 0, h, 1 - h) * rows, rows), rows)
        pltpu.make_async_copy(fresh_v.at[:, at, :], fresh_h.at[:, at, :], out_sem.at[step]).wait()


def on_device(
    video_tokens, modulation, project_weight, output_weight, norm_gains,
    text_cache, text_count, video_keep, patch_order, stale_cache,
):
    rows, width = video_tokens.shape
    patch, local = stale_cache.shape[1:]
    hd = norm_gains.shape[1]
    heads = local // hd
    text_rows = text_cache.shape[1]
    half = local // 2
    sub = rows // CHUNKS
    key_rows = 3 * patch + text_rows
    keep = video_keep.reshape(-1, hd)
    y_steps = 3
    anywhere = pl.BlockSpec(memory_space=pl.ANY)
    dma = pltpu.SemaphoreType.DMA
    vmem = pltpu.VMEM
    return pl.pallas_call(
        kernel,
        out_shape=(
            jax.ShapeDtypeStruct((rows, width), BF16),
            jax.ShapeDtypeStruct((2, patch, local), BF16),
        ),
        in_specs=[anywhere] * 10,
        out_specs=(anywhere, anywhere),
        scratch_shapes=[
            vmem((rows, width), BF16),
            vmem(modulation.shape, F32),
            vmem(project_weight.shape, BF16),
            vmem(output_weight.shape, BF16),
            vmem(norm_gains.shape, F32),
            vmem(text_cache.shape, BF16),
            vmem(keep.shape, jnp.int32),
            vmem(stale_cache.shape, BF16),
            vmem((patch, width), BF16),
            vmem((2, rows, width), BF16),
            vmem((CHUNKS, 4 * sub, width), BF16),
            vmem((2, 2, patch, half), BF16),
            vmem((2, 2, patch, half), BF16),
            vmem((patch, local), BF16),
            vmem((key_rows, local), BF16),
            vmem((key_rows, local), BF16),
            vmem((key_rows, hd), BF16),
            vmem((heads, patch, 2 * hd), F32),
            vmem((patch, local), BF16),
            vmem((patch, width), F32),
            vmem((rows, width), BF16),
            vmem((rows, width), BF16),
            vmem((2, patch, local), BF16),
            vmem((rows, width), BF16),
            pltpu.SMEM(patch_order.shape, jnp.int32),
            pltpu.SMEM(text_count.shape, jnp.int32),
            dma((11 + 2 * CHUNKS,)),
            dma((CHUNKS,)),
            dma((CHUNKS,)),
            dma((2, CHUNKS)),
            dma((2, CHUNKS)),
            dma((2, CHUNKS)),
            dma((2, CHUNKS)),
            dma((2, 2, heads // 2)),
            dma((2, 2, heads // 2)),
            dma((y_steps,)),
            dma((y_steps,)),
            dma((2 + y_steps,)),
            pltpu.SemaphoreType.REGULAR,
            pltpu.SemaphoreType.REGULAR,
        ],
        compiler_params=pltpu.CompilerParams(
            collective_id=0, has_side_effects=True, vmem_limit_bytes=60 * 1024 * 1024
        ),
        name="patch_attention",
    )(
        patch_order, text_count, video_tokens, modulation, project_weight, output_weight,
        norm_gains, text_cache, keep, stale_cache,
    )


def solution(mesh):
    placed = (
        P(("groups", "section", "head"), None),
        P("groups", None),
        P(None, None, "head"),
        P("head", None),
        P(),
        P(None, "groups", "head"),
        P("groups"),
        P("groups"),
        P("groups"),
        P(None, ("groups", "section"), "head"),
    )
    return jax.shard_map(
        on_device,
        mesh=mesh,
        in_specs=placed,
        out_specs=(P(("groups", "section", "head"), None), P(None, ("groups", "section"), "head")),
        check_vma=False,
    )
```

```python
import functools
import math

import jax
import jax.numpy as jnp
from jax import lax
from jax.experimental import pallas as pl
from jax.experimental.pallas import tpu as pltpu
from jax.sharding import PartitionSpec as P

epsilon = 1e-06
CHUNKS = 2
F32 = jnp.float32
BF16 = jnp.bfloat16
MESH = pl.DeviceIdType.MESH
NT = (((1,), (1,)), ((), ()))


def matmul(a, b):
    return jnp.dot(a, b, preferred_element_type=F32)


def head_norm(values, gain):
    square = jnp.mean(values * values, axis=-1, keepdims=True)
    return values * lax.rsqrt(square + epsilon) * gain


def kernel(
    order_h, count_h, x_h, mod_h, w_h, wo_h, gains_h, text_h, keep_h, stale_h,
    updated_h, fresh_h,
    x_v, mod_v, w_v, wo_v, gains_v, text_v, keep_v, stale_v,
    normed, message, arrived, extra, raw, q_own, kbuf, vbuf, mbuf, acc, attended, y_sum, y_out, y_in, fresh_v, updated_v, order_s, count_s,
    mask_b, kst, vst, r_out, r_in, t_out, t_in,
    load_sem, part_send, part_recv, p1_send, p1_recv, f_send, f_recv, e_send, e_recv, y_send, y_recv, out_sem,
    r_send, r_recv, t_send, t_recv, left_ready, partner_ready,
):
    rows, width = x_v.shape
    patch, local = stale_v.shape[1], stale_v.shape[2]
    text_rows = text_v.shape[1]
    hd = gains_v.shape[1]
    heads = local // hd
    half_heads = heads // 2
    half = half_heads * hd
    back = half_heads - 1
    back_cols = slice(back * hd, (back + 1) * hd)
    sub = rows // CHUNKS
    wide = 2 * hd
    sections = lax.axis_size("section")
    place = lax.axis_index("section")
    h = lax.axis_index("head")
    nbr_place = (jnp.maximum(place - 1, 0), jnp.minimum(place + 1, sections - 1))
    nbr_of = ({"section": nbr_place[0]}, {"section": nbr_place[1]})
    partner = {"head": 1 - h}
    exists = (place > 0, place < sections - 1)
    inner = (place > 0) & (place < sections - 1)

    def for_neighbour(n, work):
        pl.when(exists[n])(work)

    barrier = pltpu.get_barrier_semaphore()
    for_neighbour(0, lambda: pl.semaphore_signal(barrier, inc=1, device_id=nbr_of[0], device_id_type=MESH))

    @pl.when(h == 1)
    def _():
        pl.semaphore_signal(barrier, inc=1, device_id=partner, device_id_type=MESH)

    sources = [
        (order_h, order_s), (mod_h, mod_v), (stale_h, stale_v), (gains_h, gains_v), (keep_h, keep_v),
        (w_h.at[1], w_v.at[1]), (w_h.at[2], w_v.at[2]), (w_h.at[0], w_v.at[0]), (text_h, text_v), (wo_h, wo_v), (count_h, count_s),
    ]
    piece = sub // 2
    sources += [(x_h.at[pl.ds(i * piece, piece), :], x_v.at[pl.ds(i * piece, piece), :]) for i in range(2 * CHUNKS)]
    first_piece = len(sources) - 2 * CHUNKS
    loads = [pltpu.make_async_copy(src, dst, load_sem.at[i]) for i, (src, dst) in enumerate(sources)]
    for i in (*range(first_piece, len(loads)), *range(first_piece)):
        loads[i].start()

    one = jnp.int32(1)
    zero = jnp.int32(0)

    def full(flag, shape):
        return jnp.full(shape, flag, jnp.int32) > 0

    base = pl.multiple_of(h * rows, rows)

    def area(n, core):
        return pl.ds(pl.multiple_of((2 * n + core) * sub, sub), sub)

    def p1_copy(n, c, side):
        at = pl.ds(pl.multiple_of(c * sub, sub), sub)
        return pltpu.make_async_remote_copy(
            src_ref=message.at[n, at, :],
            dst_ref=arrived.at[c, area(side, h), :],
            send_sem=p1_send.at[n, c],
            recv_sem=p1_recv.at[side, c],
            device_id=nbr_of[n],
            device_id_type=MESH,
        )

    def extra_copy(n, kind, i, side):
        cols = slice(i * hd, (i + 1) * hd)
        return pltpu.make_async_remote_copy(
            src_ref=stale_v.at[kind, :, cols],
            dst_ref=extra.at[side, kind, :, cols],
            send_sem=e_send.at[n, kind, i],
            recv_sem=e_recv.at[side, kind, i],
            device_id=nbr_of[n],
            device_id_type=MESH,
        )

    def part_copy(c, core):
        at = pl.ds(pl.multiple_of(core * rows + c * sub, sub), sub)
        return pltpu.make_async_remote_copy(
            src_ref=normed.at[at, :],
            dst_ref=normed.at[at, :],
            send_sem=part_send.at[c],
            recv_sem=part_recv.at[c],
            device_id=partner,
            device_id_type=MESH,
        )

    def forward_copy(n, c, core):
        return pltpu.make_async_remote_copy(
            src_ref=arrived.at[c, area(n, core), :],
            dst_ref=arrived.at[c, area(n, core), :],
            send_sem=f_send.at[n, c],
            recv_sem=f_recv.at[n, c],
            device_id=partner,
            device_id_type=MESH,
        )

    def r_copy(n, c, side):
        return pltpu.make_async_remote_copy(
            src_ref=r_out.at[n, c],
            dst_ref=r_in.at[side, c],
            send_sem=r_send.at[n, c],
            recv_sem=r_recv.at[side, c],
            device_id=nbr_of[n],
            device_id_type=MESH,
        )

    def t_copy(n, c, side):
        return pltpu.make_async_remote_copy(
            src_ref=t_out.at[n, c],
            dst_ref=t_in.at[side, c],
            send_sem=t_send.at[n, c],
            recv_sem=t_recv.at[side, c],
            device_id=nbr_of[n],
            device_id_type=MESH,
        )

    extras = [(kind, i) for i in range(back) for kind in range(2)]

    def send_extras(n):
        for kind, i in extras:
            extra_copy(n, kind, i, 1 - n).start()

    def meet_left():
        pl.semaphore_wait(left_ready, 1)
        for c in range(CHUNKS):
            p1_copy(0, c, 1).start()

    def swap_parts():
        for c in range(CHUNKS):
            part_copy(c, h).start()

    def meet_right():
        needed = jnp.where(place < sections - 1, one, zero) + jnp.where(h == 0, one, zero)
        pl.when(needed > 0)(lambda: pl.semaphore_wait(barrier, needed))
        for_neighbour(1, lambda: pl.semaphore_signal(left_ready, inc=1, device_id=nbr_of[1], device_id_type=MESH))

        @pl.when(h == 0)
        def _():
            pl.semaphore_signal(partner_ready, inc=1, device_id=partner, device_id_type=MESH)

    def meet_partner():
        pl.semaphore_wait(partner_ready, 1)
        swap_parts()

    loads[1].wait()
    loads[0].wait()
    own_slot = order_s[place]
    slot = (order_s[nbr_place[0]], order_s[nbr_place[1]])
    is_b = [jnp.where(slot[n] < own_slot, one, zero) for n in range(2)]
    is_a = [jnp.where(own_slot < slot[n], one, zero) for n in range(2)]
    scale = 1.0 + mod_v[1:2, :]
    shift = mod_v[0:1, :]
    for c in range(CHUNKS):
        for p in range(2):
            at = slice(c * sub + p * piece, c * sub + (p + 1) * piece)
            loads[first_piece + 2 * c + p].wait()
            hidden = x_v[at, :].astype(F32)
            center = jnp.mean(hidden, axis=-1, keepdims=True)
            shifted = hidden - center
            spread = jnp.mean(shifted * shifted, axis=-1, keepdims=True)
            tokens = (shifted * lax.rsqrt(spread + epsilon) * scale + shift).astype(BF16)
            normed[pl.ds(pl.multiple_of(base + c * sub + p * piece, piece), piece), :] = tokens
            if c == 0 and p == 0:
                meet_right()
                loads[2].wait()
            other = slice(rows + c * sub + p * piece, rows + c * sub + (p + 1) * piece)
            packed = jnp.concatenate(
                [stale_v[0, at, half:], stale_v[0, other, half:], stale_v[1, at, half:], stale_v[1, other, half:]],
                axis=1,
            )
            for n in range(2):
                message[n, at, :] = jnp.where(full(is_a[n], tokens.shape), tokens, packed)
        for_neighbour(1, lambda c=c: p1_copy(1, c, 0).start())

    waits = (place == 1) & (h == 0)
    pl.when((place > 0) & jnp.logical_not(waits))(meet_left)
    pl.when(h == 0)(swap_parts)
    pl.when((h == 1) & (place > 0))(meet_partner)

    for i in (3, 4, 10):
        loads[i].wait()
    near = patch + text_rows

    def keep_column(index, part):
        row = keep_v[pl.ds(index * (patch // hd) + part, 1), :]
        return jnp.transpose(jnp.broadcast_to(row.astype(F32), (hd, hd))).astype(BF16)

    for part in range(patch // hd):
        low = part * hd
        mbuf[low : low + hd, :] = keep_column(place, part)
        for n in range(2):
            column = keep_column(nbr_place[n], part)
            mbuf[near + n * patch + low : near + n * patch + low + hd, :] = column
            mask_b[n * patch + low : n * patch + low + hd, :] = jnp.where(full(is_b[n], column.shape), column, 0.0)
    live = lax.broadcasted_iota(jnp.int32, (text_rows, hd), 0) < count_s[0]
    mbuf[patch:near, :] = jnp.where(live, 1.0, 0.0).astype(BF16)

    q_gain = gains_v[0:1, :] * (math.log2(math.e) * hd**-0.5)
    k_gain = gains_v[1:2, :]
    t_gain = gains_v[2:3, :]

    def own(at, index, beside):
        for i in range(local // wide):
            block = slice(i * wide, (i + 1) * wide)
            result = matmul(normed[at, :], w_v[index, :, block])
            if index > 0:
                result = result.astype(BF16)
                fresh_v[index - 1, at, block] = result
            for j in range(2):
                lanes = slice(j * hd, (j + 1) * hd)
                cols = slice(i * wide + j * hd, i * wide + (j + 1) * hd)
                if index == 0:
                    q_own[at, cols] = head_norm(result[:, lanes], q_gain).astype(BF16)
                if index == 1:
                    kbuf[at, cols] = head_norm(result[:, lanes].astype(F32), k_gain).astype(BF16)
                if index == 2:
                    vbuf[at, cols] = result[:, lanes] * mbuf[at, :]
                if beside:
                    kbuf[patch:near, cols] = head_norm(text_v[0, :, cols].astype(F32), t_gain).astype(BF16)
                    vbuf[patch:near, cols] = text_v[1, :, cols] * mbuf[patch:near, :]

    for step in range(2):
        side = h if step == 0 else 1 - h
        at = pl.ds(pl.multiple_of(side * rows, rows), rows)
        if step == 1:
            for_neighbour(1, lambda: send_extras(1))
            pl.when((h == 1) & (place == 0))(meet_partner)
            pl.when((place > 0) & jnp.logical_not(waits))(lambda: send_extras(0))
            for c in range(CHUNKS):
                part_copy(c, 1 - h).wait_recv()
        if step == 0:
            loads[5].wait()
            loads[6].wait()
        else:
            loads[8].wait()
        own(at, 1, step == 1)
        own(at, 2, False)
        if step == 0:
            loads[7].wait()
        else:
            kst[...] = head_norm(stale_v[0, :, back_cols].astype(F32), k_gain).astype(BF16)
            vst[...] = stale_v[1, :, back_cols] * mbuf[:patch, :]
        own(at, 0, False)
        pltpu.make_async_copy(fresh_v.at[:, at, :], fresh_h.at[:, at, :], out_sem.at[step]).start()

    def take(n, c):
        p1_copy(n, c, n).wait_recv()
        forward_copy(n, c, h).start()

    def scores(query, key):
        return lax.dot_general(query, key, NT, preferred_element_type=F32)

    def attend(at, i):
        cols = slice(i * hd, (i + 1) * hd)
        weight = jnp.exp2(scores(q_own[:, cols], kbuf[at, cols])).astype(BF16)
        return matmul(weight, jnp.concatenate([vbuf[at, cols], mbuf[at, :]], axis=1))

    pl.when(place == 0)(lambda: take(1, 0))
    for i in range(half_heads):
        acc[i] = attend(slice(0, near), i)

    def own_rest():
        for i in range(half_heads, heads):
            acc[i] = attend(slice(0, near), i)

    pl.when(place > 0)(own_rest)

    def job(n, c):
        forward_copy(n, c, 1 - h).wait_recv()
        tokens = arrived.at[c, pl.ds(2 * n * sub, 2 * sub), :]
        pick = full(is_b[n], (sub, hd))

        def project(i):
            block = slice(i * wide, (i + 1) * wide)
            for kind in range(2):
                result = matmul(tokens[...], w_v[1 + kind, :, block]).astype(BF16)
                for j in range(2):
                    head = 2 * i + j
                    cols = slice(head * hd, (head + 1) * hd)
                    for core in range(2):
                        part = result[core * sub : (core + 1) * sub, j * hd : (j + 1) * hd]
                        row = pl.multiple_of(core * rows + c * sub, sub)
                        if head == back:
                            to = pl.ds(pl.multiple_of(near + n * patch + row, sub), sub)
                            if kind == 0:
                                kbuf[to, cols] = head_norm(part.astype(F32), k_gain).astype(BF16)
                            else:
                                vbuf[to, cols] = part * mask_b[pl.ds(pl.multiple_of(n * patch + row, sub), sub), :]
                            continue
                        if head < half_heads:
                            raw[n, kind, pl.ds(row, sub), cols] = part
                            continue
                        low = (2 * kind + core) * half + (head - half_heads) * hd
                        part = jnp.where(pick, part, arrived[c, area(n, h), low : low + hd])
                        to = pl.ds(pl.multiple_of(near + n * patch + row, sub), sub)
                        if kind == 0:
                            kbuf[to, cols] = head_norm(part.astype(F32), k_gain).astype(BF16)
                        else:
                            vbuf[to, cols] = part * mbuf[to, :]
        blocks = local // wide
        query = matmul(tokens[...], w_v[0, :, back_cols])
        project(blocks - 1)
        query = head_norm(query, q_gain).astype(BF16)
        score = scores(query, kst[...])
        for i in range(1, blocks - 1):
            project(i)
        weight = jnp.exp2(score).astype(BF16)
        both = matmul(weight, jnp.concatenate([vst[...], mbuf[:patch, :]], axis=1))
        project(0)
        r_out[n, c] = both[:, :hd].astype(BF16)
        for p in range(2 * sub // hd):
            t_out[n, c, 0:1, p * hd : (p + 1) * hd] = jnp.transpose(both[p * hd : (p + 1) * hd, hd:])[0:1, :]
        r_copy(n, c, 1 - n).start()
        t_copy(n, c, 1 - n).start()

    def jobs(t, carry):
        delay = jnp.where(place == 1, CHUNKS, 0)
        has_right = exists[1] & (t < CHUNKS)
        has_left = exists[0] & (t >= delay) & (t < delay + CHUNKS)

        @pl.when(waits & (t == 1))
        def _():
            meet_left()
            send_extras(0)

        pl.when(has_right & (place > 0))(lambda: take(1, t))
        pl.when(has_left)(lambda: take(0, t - delay))

        pl.when(has_right)(lambda: job(1, t))

        @pl.when((place == 0) & (t == 0))
        def _():
            for c in range(1, CHUNKS):
                take(1, c)
            own_rest()

        pl.when(has_left)(lambda: job(0, t - delay))
        return carry

    lax.fori_loop(0, 2 * CHUNKS, jobs, 0)

    def finish_head(at, i):
        cols = slice(i * hd, (i + 1) * hd)
        both = acc[i] + attend(at, i)
        attended[:, cols] = (both[:, :hd] / both[:, hd:]).astype(BF16)

    def finish_heads(which):
        @pl.when(inner)
        def _():
            for i in which:
                finish_head(slice(near, near + 2 * patch), i)

        @pl.when(jnp.logical_not(inner))
        def _():
            at = pl.ds(pl.multiple_of(near + jnp.where(place > 0, 0, patch), 2 * sub), patch)
            for i in which:
                finish_head(at, i)

    def back_head(at, b_at):
        weight = jnp.exp2(scores(q_own[:, back_cols], kbuf[at, back_cols])).astype(BF16)
        acc[back] += matmul(weight, jnp.concatenate([vbuf[at, back_cols], mask_b[b_at, :]], axis=1))

    def start_back():
        @pl.when(inner)
        def _():
            back_head(slice(near, near + 2 * patch), slice(0, 2 * patch))

        @pl.when(jnp.logical_not(inner))
        def _():
            only = jnp.where(place > 0, 0, patch)
            at = pl.ds(pl.multiple_of(near + only, 2 * sub), patch)
            back_head(at, pl.ds(pl.multiple_of(only, patch), patch))

    def add_back(n):
        for c in range(CHUNKS):
            r_copy(n, c, n).wait_recv()
            t_copy(n, c, n).wait_recv()
            for core in range(2):
                spot = pl.ds(core * rows + c * sub, sub)
                part = slice(core * sub, (core + 1) * sub)
                total = jnp.transpose(jnp.broadcast_to(t_in[n, c, 0:1, part], (hd, sub)))
                pick = full(is_a[n], total.shape)
                acc[back, spot, :hd] += jnp.where(pick, r_in[n, c, part, :].astype(F32), 0.0)
                acc[back, spot, hd:] += jnp.where(pick, total, 0.0)

    def take_extra(n, i):
        for kind in range(2):
            extra_copy(n, kind, i, n).wait_recv()
        cols = slice(i * hd, (i + 1) * hd)
        pick = full(is_b[n], (patch, hd))
        to = slice(near + n * patch, near + (n + 1) * patch)
        k_part = jnp.where(pick, raw[n, 0, :, cols], extra[n, 0, :, cols])
        v_part = jnp.where(pick, raw[n, 1, :, cols], extra[n, 1, :, cols])
        kbuf[to, cols] = head_norm(k_part.astype(F32), k_gain).astype(BF16)
        vbuf[to, cols] = v_part * mbuf[to, :]

    def extra_head(i):
        for n in (1, 0):
            for_neighbour(n, lambda n=n: take_extra(n, i))
        finish_heads([i])

    steps = y_send.shape[0]
    span = width // steps

    def partial_sum(pair, first):
        lanes = slice(pair * wide, (pair + 1) * wide)
        for s in range(steps):
            cols = slice(s * span, (s + 1) * span)
            part = matmul(attended[:, lanes], wo_v[lanes, cols])
            y_sum[:, cols] = part if first else y_sum[:, cols] + part

    finish_heads(range(half_heads, heads))
    start_back()
    loads[9].wait()
    last = (half_heads - 1) // 2
    late_pairs = [pair for pair in range(heads // 2) if 2 * pair + 1 < half_heads]
    early_pairs = [pair for pair in range(heads // 2) if 2 * pair >= half_heads]
    for k, pair in enumerate(early_pairs):
        partial_sum(pair, k == 0)
    for i in range(back):
        extra_head(i)
    for pair in late_pairs:
        partial_sum(pair, False)
    for n in (1, 0):
        for_neighbour(n, lambda n=n: add_back(n))
    attended[:, back_cols] = (acc[back, :, :hd] / acc[back, :, hd:]).astype(BF16)

    lanes = slice(last * wide, (last + 1) * wide)
    other = pl.ds(pl.multiple_of((1 - h) * rows, rows), rows)
    mine = pl.ds(base, rows)

    def y_copy(s):
        cols = slice(s * span, (s + 1) * span)
        return pltpu.make_async_remote_copy(
            src_ref=y_out.at[:, cols],
            dst_ref=y_in.at[:, cols],
            send_sem=y_send.at[s],
            recv_sem=y_recv.at[s],
            device_id=partner,
            device_id_type=MESH,
        )

    for s in range(steps):
        cols = slice(s * span, (s + 1) * span)
        y_out[:, cols] = (y_sum[other, cols] + matmul(attended[other, lanes], wo_v[lanes, cols])).astype(BF16)
        y_copy(s).start()
    for s in range(steps):
        cols = slice(s * span, (s + 1) * span)
        y_sum[mine, cols] += matmul(attended[mine, lanes], wo_v[lanes, cols])
    for s in range(steps):
        cols = slice(s * span, (s + 1) * span)
        y_copy(s).wait_recv()
        mixed = y_sum[mine, cols] + y_in[:, cols].astype(F32)
        updated_v[:, cols] = (x_v[:, cols].astype(F32) + mod_v[2:3, cols] * mixed).astype(BF16)
        pltpu.make_async_copy(updated_v.at[:, cols], updated_h.at[:, cols], out_sem.at[2 + s]).start()

    def sent_to(n):
        for c in range(CHUNKS):
            p1_copy(n, c, 1 - n).wait_send()
            forward_copy(n, c, h).wait_send()
            r_copy(n, c, 1 - n).wait_send()
            t_copy(n, c, 1 - n).wait_send()
        for kind, i in extras:
            extra_copy(n, kind, i, 1 - n).wait_send()

    for n in range(2):
        for_neighbour(n, lambda n=n: sent_to(n))
    for c in range(CHUNKS):
        part_copy(c, h).wait_send()
    for s in range(steps):
        y_copy(s).wait_send()
        cols = slice(s * span, (s + 1) * span)
        pltpu.make_async_copy(updated_v.at[:, cols], updated_h.at[:, cols], out_sem.at[2 + s]).wait()
    for step in range(2):
        at = pl.ds(pl.multiple_of(jnp.where(step == 0, h, 1 - h) * rows, rows), rows)
        pltpu.make_async_copy(fresh_v.at[:, at, :], fresh_h.at[:, at, :], out_sem.at[step]).wait()


def on_device(
    video_tokens, modulation, project_weight, output_weight, norm_gains,
    text_cache, text_count, video_keep, patch_order, stale_cache,
):
    rows, width = video_tokens.shape
    patch, local = stale_cache.shape[1:]
    hd = norm_gains.shape[1]
    heads = local // hd
    text_rows = text_cache.shape[1]
    half = local // 2
    sub = rows // CHUNKS
    key_rows = 3 * patch + text_rows
    keep = video_keep.reshape(-1, hd)
    y_steps = 3
    anywhere = pl.BlockSpec(memory_space=pl.ANY)
    dma = pltpu.SemaphoreType.DMA
    vmem = pltpu.VMEM
    return pl.pallas_call(
        kernel,
        out_shape=(
            jax.ShapeDtypeStruct((rows, width), BF16),
            jax.ShapeDtypeStruct((2, patch, local), BF16),
        ),
        in_specs=[anywhere] * 10,
        out_specs=(anywhere, anywhere),
        scratch_shapes=[
            vmem((rows, width), BF16),
            vmem(modulation.shape, F32),
            vmem(project_weight.shape, BF16),
            vmem(output_weight.shape, BF16),
            vmem(norm_gains.shape, F32),
            vmem(text_cache.shape, BF16),
            vmem(keep.shape, jnp.int32),
            vmem(stale_cache.shape, BF16),
            vmem((patch, width), BF16),
            vmem((2, rows, width), BF16),
            vmem((CHUNKS, 4 * sub, width), BF16),
            vmem((2, 2, patch, half), BF16),
            vmem((2, 2, patch, half), BF16),
            vmem((patch, local), BF16),
            vmem((key_rows, local), BF16),
            vmem((key_rows, local), BF16),
            vmem((key_rows, hd), BF16),
            vmem((heads, patch, 2 * hd), F32),
            vmem((patch, local), BF16),
            vmem((patch, width), F32),
            vmem((rows, width), BF16),
            vmem((rows, width), BF16),
            vmem((2, patch, local), BF16),
            vmem((rows, width), BF16),
            pltpu.SMEM(patch_order.shape, jnp.int32),
            pltpu.SMEM(text_count.shape, jnp.int32),
            vmem((2 * patch, hd), BF16),
            vmem((patch, hd), BF16),
            vmem((patch, hd), BF16),
            vmem((2, CHUNKS, 2 * sub, hd), BF16),
            vmem((2, CHUNKS, 2 * sub, hd), BF16),
            vmem((2, CHUNKS, 8, 2 * sub), F32),
            vmem((2, CHUNKS, 8, 2 * sub), F32),
            dma((11 + 2 * CHUNKS,)),
            dma((CHUNKS,)),
            dma((CHUNKS,)),
            dma((2, CHUNKS)),
            dma((2, CHUNKS)),
            dma((2, CHUNKS)),
            dma((2, CHUNKS)),
            dma((2, 2, heads // 2)),
            dma((2, 2, heads // 2)),
            dma((y_steps,)),
            dma((y_steps,)),
            dma((2 + y_steps,)),
            dma((2, CHUNKS)),
            dma((2, CHUNKS)),
            dma((2, CHUNKS)),
            dma((2, CHUNKS)),
            pltpu.SemaphoreType.REGULAR,
            pltpu.SemaphoreType.REGULAR,
        ],
        compiler_params=pltpu.CompilerParams(
            collective_id=0, has_side_effects=True, vmem_limit_bytes=60 * 1024 * 1024
        ),
        name="patch_attention",
    )(
        patch_order, text_count, video_tokens, modulation, project_weight, output_weight,
        norm_gains, text_cache, keep, stale_cache,
    )


def solution(mesh):
    placed = (
        P(("groups", "section", "head"), None),
        P("groups", None),
        P(None, None, "head"),
        P("head", None),
        P(),
        P(None, "groups", "head"),
        P("groups"),
        P("groups"),
        P("groups"),
        P(None, ("groups", "section"), "head"),
    )
    return jax.shard_map(
        on_device,
        mesh=mesh,
        in_specs=placed,
        out_specs=(P(("groups", "section", "head"), None), P(None, ("groups", "section"), "head")),
        check_vma=False,
    )
```

```python
import functools
import math

import jax
import jax.numpy as jnp
from jax import lax
from jax.experimental import pallas as pl
from jax.experimental.pallas import tpu as pltpu
from jax.sharding import PartitionSpec as P

epsilon = 1e-06
CHUNKS = 2
F32 = jnp.float32
BF16 = jnp.bfloat16
MESH = pl.DeviceIdType.MESH
NT = (((1,), (1,)), ((), ()))


def matmul(a, b):
    return jnp.dot(a, b, preferred_element_type=F32)


def head_norm(values, gain):
    square = jnp.mean(values * values, axis=-1, keepdims=True)
    return values * lax.rsqrt(square + epsilon) * gain


def kernel(
    order_h, count_h, x_h, mod_h, w_h, wo_h, gains_h, text_h, keep_h, stale_h,
    updated_h, fresh_h,
    x_v, mod_v, w_v, wo_v, gains_v, text_v, keep_v, stale_v,
    normed, message, arrived, extra, raw, q_own, kbuf, vbuf, mbuf, acc, attended, y_sum, y_out, y_in, fresh_v, updated_v, order_s, count_s,
    mask_b, kst, vst, r_out, r_in, t_out, t_in,
    load_sem, part_send, part_recv, p1_send, p1_recv, f_send, f_recv, e_send, e_recv, y_send, y_recv, out_sem,
    r_send, r_recv, t_send, t_recv, left_ready, partner_ready,
):
    rows, width = x_v.shape
    patch, local = stale_v.shape[1], stale_v.shape[2]
    text_rows = text_v.shape[1]
    hd = gains_v.shape[1]
    heads = local // hd
    half_heads = heads // 2
    half = half_heads * hd
    back = half_heads - 1
    back_cols = slice(back * hd, (back + 1) * hd)
    sub = rows // CHUNKS
    wide = 2 * hd
    sections = lax.axis_size("section")
    place = lax.axis_index("section")
    h = lax.axis_index("head")
    nbr_place = (jnp.maximum(place - 1, 0), jnp.minimum(place + 1, sections - 1))
    nbr_of = ({"section": nbr_place[0]}, {"section": nbr_place[1]})
    partner = {"head": 1 - h}
    exists = (place > 0, place < sections - 1)
    inner = (place > 0) & (place < sections - 1)

    def for_neighbour(n, work):
        pl.when(exists[n])(work)

    barrier = pltpu.get_barrier_semaphore()
    for_neighbour(0, lambda: pl.semaphore_signal(barrier, inc=1, device_id=nbr_of[0], device_id_type=MESH))

    @pl.when(h == 1)
    def _():
        pl.semaphore_signal(barrier, inc=1, device_id=partner, device_id_type=MESH)

    sources = [
        (order_h, order_s), (mod_h, mod_v), (stale_h, stale_v), (gains_h, gains_v), (keep_h, keep_v),
        (w_h.at[1], w_v.at[1]), (w_h.at[2], w_v.at[2]), (w_h.at[0], w_v.at[0]), (text_h, text_v), (wo_h, wo_v), (count_h, count_s),
    ]
    piece = sub // 2
    sources += [(x_h.at[pl.ds(i * piece, piece), :], x_v.at[pl.ds(i * piece, piece), :]) for i in range(2 * CHUNKS)]
    first_piece = len(sources) - 2 * CHUNKS
    loads = [pltpu.make_async_copy(src, dst, load_sem.at[i]) for i, (src, dst) in enumerate(sources)]
    for i in (*range(first_piece, len(loads)), *range(first_piece)):
        loads[i].start()

    one = jnp.int32(1)
    zero = jnp.int32(0)

    def full(flag, shape):
        return jnp.full(shape, flag, jnp.int32) > 0

    base = pl.multiple_of(h * rows, rows)

    def area(n, core):
        return pl.ds(pl.multiple_of((2 * n + core) * sub, sub), sub)

    def p1_copy(n, c, side):
        at = pl.ds(pl.multiple_of(c * sub, sub), sub)
        return pltpu.make_async_remote_copy(
            src_ref=message.at[n, at, :],
            dst_ref=arrived.at[c, area(side, h), :],
            send_sem=p1_send.at[n, c],
            recv_sem=p1_recv.at[side, c],
            device_id=nbr_of[n],
            device_id_type=MESH,
        )

    def extra_copy(n, kind, i, side):
        cols = slice(i * hd, (i + 1) * hd)
        return pltpu.make_async_remote_copy(
            src_ref=stale_v.at[kind, :, cols],
            dst_ref=extra.at[side, kind, :, cols],
            send_sem=e_send.at[n, kind, i],
            recv_sem=e_recv.at[side, kind, i],
            device_id=nbr_of[n],
            device_id_type=MESH,
        )

    def part_copy(c, core):
        at = pl.ds(pl.multiple_of(core * rows + c * sub, sub), sub)
        return pltpu.make_async_remote_copy(
            src_ref=normed.at[at, :],
            dst_ref=normed.at[at, :],
            send_sem=part_send.at[c],
            recv_sem=part_recv.at[c],
            device_id=partner,
            device_id_type=MESH,
        )

    def forward_copy(n, c, core):
        return pltpu.make_async_remote_copy(
            src_ref=arrived.at[c, area(n, core), :],
            dst_ref=arrived.at[c, area(n, core), :],
            send_sem=f_send.at[n, c],
            recv_sem=f_recv.at[n, c],
            device_id=partner,
            device_id_type=MESH,
        )

    def r_copy(n, c, side):
        return pltpu.make_async_remote_copy(
            src_ref=r_out.at[n, c],
            dst_ref=r_in.at[side, c],
            send_sem=r_send.at[n, c],
            recv_sem=r_recv.at[side, c],
            device_id=nbr_of[n],
            device_id_type=MESH,
        )

    def t_copy(n, c, side):
        return pltpu.make_async_remote_copy(
            src_ref=t_out.at[n, c],
            dst_ref=t_in.at[side, c],
            send_sem=t_send.at[n, c],
            recv_sem=t_recv.at[side, c],
            device_id=nbr_of[n],
            device_id_type=MESH,
        )

    extras = [(kind, i) for i in range(back) for kind in range(2)]

    def send_extras(n):
        for kind, i in extras:
            extra_copy(n, kind, i, 1 - n).start()

    def meet_left():
        pl.semaphore_wait(left_ready, 1)
        for c in range(CHUNKS):
            p1_copy(0, c, 1).start()

    def swap_parts():
        for c in range(CHUNKS):
            part_copy(c, h).start()

    def meet_right():
        needed = jnp.where(place < sections - 1, one, zero) + jnp.where(h == 0, one, zero)
        pl.when(needed > 0)(lambda: pl.semaphore_wait(barrier, needed))
        for_neighbour(1, lambda: pl.semaphore_signal(left_ready, inc=1, device_id=nbr_of[1], device_id_type=MESH))

        @pl.when(h == 0)
        def _():
            pl.semaphore_signal(partner_ready, inc=1, device_id=partner, device_id_type=MESH)

    def meet_partner():
        pl.semaphore_wait(partner_ready, 1)
        swap_parts()

    pl.when(place == 0)(meet_right)

    loads[1].wait()
    loads[0].wait()
    own_slot = order_s[place]
    slot = (order_s[nbr_place[0]], order_s[nbr_place[1]])
    is_b = [jnp.where(slot[n] < own_slot, one, zero) for n in range(2)]
    is_a = [jnp.where(own_slot < slot[n], one, zero) for n in range(2)]
    scale = 1.0 + mod_v[1:2, :]
    shift = mod_v[0:1, :]
    for c in range(CHUNKS):
        for p in range(2):
            at = slice(c * sub + p * piece, c * sub + (p + 1) * piece)
            loads[first_piece + 2 * c + p].wait()
            hidden = x_v[at, :].astype(F32)
            center = jnp.mean(hidden, axis=-1, keepdims=True)
            shifted = hidden - center
            spread = jnp.mean(shifted * shifted, axis=-1, keepdims=True)
            tokens = (shifted * lax.rsqrt(spread + epsilon) * scale + shift).astype(BF16)
            normed[pl.ds(pl.multiple_of(base + c * sub + p * piece, piece), piece), :] = tokens
            if c == 0 and p == 0:
                pl.when(place > 0)(meet_right)
                loads[2].wait()
            other = slice(rows + c * sub + p * piece, rows + c * sub + (p + 1) * piece)
            packed = jnp.concatenate(
                [stale_v[0, at, half:], stale_v[0, other, half:], stale_v[1, at, half:], stale_v[1, other, half:]],
                axis=1,
            )
            for n in range(2):
                message[n, at, :] = jnp.where(full(is_a[n], tokens.shape), tokens, packed)
        for_neighbour(1, lambda c=c: p1_copy(1, c, 0).start())

    waits = (place == 1) & (h == 0)
    pl.when((place > 0) & jnp.logical_not(waits))(meet_left)
    pl.when(h == 0)(swap_parts)
    pl.when((h == 1) & (place > 0))(meet_partner)

    for i in (3, 4, 10):
        loads[i].wait()
    near = patch + text_rows

    def keep_column(index, part):
        row = keep_v[pl.ds(index * (patch // hd) + part, 1), :]
        return jnp.transpose(jnp.broadcast_to(row.astype(F32), (hd, hd))).astype(BF16)

    for part in range(patch // hd):
        low = part * hd
        mbuf[low : low + hd, :] = keep_column(place, part)
        for n in range(2):
            column = keep_column(nbr_place[n], part)
            mbuf[near + n * patch + low : near + n * patch + low + hd, :] = column
            mask_b[n * patch + low : n * patch + low + hd, :] = jnp.where(full(is_b[n], column.shape), column, 0.0)
    live = lax.broadcasted_iota(jnp.int32, (text_rows, hd), 0) < count_s[0]
    mbuf[patch:near, :] = jnp.where(live, 1.0, 0.0).astype(BF16)

    q_gain = gains_v[0:1, :] * (math.log2(math.e) * hd**-0.5)
    k_gain = gains_v[1:2, :]
    t_gain = gains_v[2:3, :]

    def own(at, index, beside):
        for i in range(local // wide):
            block = slice(i * wide, (i + 1) * wide)
            result = matmul(normed[at, :], w_v[index, :, block])
            if index > 0:
                result = result.astype(BF16)
                fresh_v[index - 1, at, block] = result
            for j in range(2):
                lanes = slice(j * hd, (j + 1) * hd)
                cols = slice(i * wide + j * hd, i * wide + (j + 1) * hd)
                if index == 0:
                    q_own[at, cols] = head_norm(result[:, lanes], q_gain).astype(BF16)
                if index == 1:
                    kbuf[at, cols] = head_norm(result[:, lanes].astype(F32), k_gain).astype(BF16)
                if index == 2:
                    vbuf[at, cols] = result[:, lanes] * mbuf[at, :]
                if beside:
                    kbuf[patch:near, cols] = head_norm(text_v[0, :, cols].astype(F32), t_gain).astype(BF16)
                    vbuf[patch:near, cols] = text_v[1, :, cols] * mbuf[patch:near, :]

    for step in range(2):
        side = h if step == 0 else 1 - h
        at = pl.ds(pl.multiple_of(side * rows, rows), rows)
        if step == 1:
            for_neighbour(1, lambda: send_extras(1))
            pl.when((h == 1) & (place == 0))(meet_partner)
            pl.when((place > 0) & jnp.logical_not(waits))(lambda: send_extras(0))
            for c in range(CHUNKS):
                part_copy(c, 1 - h).wait_recv()
        if step == 0:
            loads[5].wait()
            loads[6].wait()
        else:
            loads[8].wait()
        own(at, 1, step == 1)
        own(at, 2, False)
        if step == 0:
            loads[7].wait()
        else:
            kst[...] = head_norm(stale_v[0, :, back_cols].astype(F32), k_gain).astype(BF16)
            vst[...] = stale_v[1, :, back_cols] * mbuf[:patch, :]
        own(at, 0, False)
        pltpu.make_async_copy(fresh_v.at[:, at, :], fresh_h.at[:, at, :], out_sem.at[step]).start()

    def take(n, c):
        p1_copy(n, c, n).wait_recv()
        forward_copy(n, c, h).start()

    def scores(query, key):
        return lax.dot_general(query, key, NT, preferred_element_type=F32)

    def attend(at, i):
        cols = slice(i * hd, (i + 1) * hd)
        weight = jnp.exp2(scores(q_own[:, cols], kbuf[at, cols])).astype(BF16)
        return matmul(weight, jnp.concatenate([vbuf[at, cols], mbuf[at, :]], axis=1))

    pl.when(place == 0)(lambda: take(1, 0))
    for i in range(half_heads):
        acc[i] = attend(slice(0, near), i)

    def own_rest():
        for i in range(half_heads, heads):
            acc[i] = attend(slice(0, near), i)

    pl.when(place > 0)(own_rest)

    def job(n, c):
        forward_copy(n, c, 1 - h).wait_recv()
        tokens = arrived.at[c, pl.ds(2 * n * sub, 2 * sub), :]
        pick = full(is_b[n], (sub, hd))

        def project(i):
            block = slice(i * wide, (i + 1) * wide)
            for kind in range(2):
                result = matmul(tokens[...], w_v[1 + kind, :, block]).astype(BF16)
                for j in range(2):
                    head = 2 * i + j
                    cols = slice(head * hd, (head + 1) * hd)
                    for core in range(2):
                        part = result[core * sub : (core + 1) * sub, j * hd : (j + 1) * hd]
                        row = pl.multiple_of(core * rows + c * sub, sub)
                        if head == back:
                            to = pl.ds(pl.multiple_of(near + n * patch + row, sub), sub)
                            if kind == 0:
                                kbuf[to, cols] = head_norm(part.astype(F32), k_gain).astype(BF16)
                            else:
                                vbuf[to, cols] = part * mask_b[pl.ds(pl.multiple_of(n * patch + row, sub), sub), :]
                            continue
                        if head < half_heads:
                            raw[n, kind, pl.ds(row, sub), cols] = part
                            continue
                        low = (2 * kind + core) * half + (head - half_heads) * hd
                        part = jnp.where(pick, part, arrived[c, area(n, h), low : low + hd])
                        to = pl.ds(pl.multiple_of(near + n * patch + row, sub), sub)
                        if kind == 0:
                            kbuf[to, cols] = head_norm(part.astype(F32), k_gain).astype(BF16)
                        else:
                            vbuf[to, cols] = part * mbuf[to, :]
        blocks = local // wide
        query = matmul(tokens[...], w_v[0, :, back_cols])
        project(blocks - 1)
        query = head_norm(query, q_gain).astype(BF16)
        score = scores(query, kst[...])
        for i in range(1, blocks - 1):
            project(i)
        weight = jnp.exp2(score).astype(BF16)
        both = matmul(weight, jnp.concatenate([vst[...], mbuf[:patch, :]], axis=1))
        project(0)
        r_out[n, c] = both[:, :hd].astype(BF16)
        for p in range(2 * sub // hd):
            t_out[n, c, 0:1, p * hd : (p + 1) * hd] = jnp.transpose(both[p * hd : (p + 1) * hd, hd:])[0:1, :]
        r_copy(n, c, 1 - n).start()
        t_copy(n, c, 1 - n).start()

    def jobs(t, carry):
        delay = jnp.where(place == 1, CHUNKS, 0)
        has_right = exists[1] & (t < CHUNKS)
        has_left = exists[0] & (t >= delay) & (t < delay + CHUNKS)

        @pl.when(waits & (t == 1))
        def _():
            meet_left()
            send_extras(0)

        pl.when(has_right & (place > 0))(lambda: take(1, t))
        pl.when(has_left)(lambda: take(0, t - delay))

        pl.when(has_right)(lambda: job(1, t))

        @pl.when((place == 0) & (t == 0))
        def _():
            for c in range(1, CHUNKS):
                take(1, c)
            own_rest()

        pl.when(has_left)(lambda: job(0, t - delay))
        return carry

    lax.fori_loop(0, 2 * CHUNKS, jobs, 0)

    def finish_head(at, i):
        cols = slice(i * hd, (i + 1) * hd)
        both = acc[i] + attend(at, i)
        attended[:, cols] = (both[:, :hd] / both[:, hd:]).astype(BF16)

    def finish_heads(which):
        @pl.when(inner)
        def _():
            for i in which:
                finish_head(slice(near, near + 2 * patch), i)

        @pl.when(jnp.logical_not(inner))
        def _():
            at = pl.ds(pl.multiple_of(near + jnp.where(place > 0, 0, patch), 2 * sub), patch)
            for i in which:
                finish_head(at, i)

    def back_head(at, b_at):
        weight = jnp.exp2(scores(q_own[:, back_cols], kbuf[at, back_cols])).astype(BF16)
        acc[back] += matmul(weight, jnp.concatenate([vbuf[at, back_cols], mask_b[b_at, :]], axis=1))

    def start_back():
        @pl.when(inner)
        def _():
            back_head(slice(near, near + 2 * patch), slice(0, 2 * patch))

        @pl.when(jnp.logical_not(inner))
        def _():
            only = jnp.where(place > 0, 0, patch)
            at = pl.ds(pl.multiple_of(near + only, 2 * sub), patch)
            back_head(at, pl.ds(pl.multiple_of(only, patch), patch))

    def add_back(n):
        for c in range(CHUNKS):
            r_copy(n, c, n).wait_recv()
            t_copy(n, c, n).wait_recv()
            for core in range(2):
                spot = pl.ds(core * rows + c * sub, sub)
                part = slice(core * sub, (core + 1) * sub)
                total = jnp.transpose(jnp.broadcast_to(t_in[n, c, 0:1, part], (hd, sub)))
                pick = full(is_a[n], total.shape)
                acc[back, spot, :hd] += jnp.where(pick, r_in[n, c, part, :].astype(F32), 0.0)
                acc[back, spot, hd:] += jnp.where(pick, total, 0.0)

    def take_extra(n, i):
        for kind in range(2):
            extra_copy(n, kind, i, n).wait_recv()
        cols = slice(i * hd, (i + 1) * hd)
        pick = full(is_b[n], (patch, hd))
        to = slice(near + n * patch, near + (n + 1) * patch)
        k_part = jnp.where(pick, raw[n, 0, :, cols], extra[n, 0, :, cols])
        v_part = jnp.where(pick, raw[n, 1, :, cols], extra[n, 1, :, cols])
        kbuf[to, cols] = head_norm(k_part.astype(F32), k_gain).astype(BF16)
        vbuf[to, cols] = v_part * mbuf[to, :]

    def extra_head(i):
        for n in (1, 0):
            for_neighbour(n, lambda n=n: take_extra(n, i))
        finish_heads([i])

    steps = y_send.shape[0]
    span = width // steps

    def partial_sum(pair, first):
        lanes = slice(pair * wide, (pair + 1) * wide)
        for s in range(steps):
            cols = slice(s * span, (s + 1) * span)
            part = matmul(attended[:, lanes], wo_v[lanes, cols])
            y_sum[:, cols] = part if first else y_sum[:, cols] + part

    finish_heads(range(half_heads, heads))
    start_back()
    loads[9].wait()
    last = (half_heads - 1) // 2
    late_pairs = [pair for pair in range(heads // 2) if 2 * pair + 1 < half_heads]
    early_pairs = [pair for pair in range(heads // 2) if 2 * pair >= half_heads]
    for k, pair in enumerate(early_pairs):
        partial_sum(pair, k == 0)
    for i in range(back):
        extra_head(i)
    for pair in late_pairs:
        partial_sum(pair, False)
    for n in (1, 0):
        for_neighbour(n, lambda n=n: add_back(n))
    attended[:, back_cols] = (acc[back, :, :hd] / acc[back, :, hd:]).astype(BF16)

    lanes = slice(last * wide, (last + 1) * wide)
    other = pl.ds(pl.multiple_of((1 - h) * rows, rows), rows)
    mine = pl.ds(base, rows)

    def y_copy(s):
        cols = slice(s * span, (s + 1) * span)
        return pltpu.make_async_remote_copy(
            src_ref=y_out.at[:, cols],
            dst_ref=y_in.at[:, cols],
            send_sem=y_send.at[s],
            recv_sem=y_recv.at[s],
            device_id=partner,
            device_id_type=MESH,
        )

    for s in range(steps):
        cols = slice(s * span, (s + 1) * span)
        y_out[:, cols] = (y_sum[other, cols] + matmul(attended[other, lanes], wo_v[lanes, cols])).astype(BF16)
        y_copy(s).start()
    for s in range(steps):
        cols = slice(s * span, (s + 1) * span)
        y_sum[mine, cols] += matmul(attended[mine, lanes], wo_v[lanes, cols])
    for s in range(steps):
        cols = slice(s * span, (s + 1) * span)
        y_copy(s).wait_recv()
        mixed = y_sum[mine, cols] + y_in[:, cols].astype(F32)
        updated_v[:, cols] = (x_v[:, cols].astype(F32) + mod_v[2:3, cols] * mixed).astype(BF16)
        pltpu.make_async_copy(updated_v.at[:, cols], updated_h.at[:, cols], out_sem.at[2 + s]).start()

    def sent_to(n):
        for c in range(CHUNKS):
            p1_copy(n, c, 1 - n).wait_send()
            forward_copy(n, c, h).wait_send()
            r_copy(n, c, 1 - n).wait_send()
            t_copy(n, c, 1 - n).wait_send()
        for kind, i in extras:
            extra_copy(n, kind, i, 1 - n).wait_send()

    for n in range(2):
        for_neighbour(n, lambda n=n: sent_to(n))
    for c in range(CHUNKS):
        part_copy(c, h).wait_send()
    for s in range(steps):
        y_copy(s).wait_send()
        cols = slice(s * span, (s + 1) * span)
        pltpu.make_async_copy(updated_v.at[:, cols], updated_h.at[:, cols], out_sem.at[2 + s]).wait()
    for step in range(2):
        at = pl.ds(pl.multiple_of(jnp.where(step == 0, h, 1 - h) * rows, rows), rows)
        pltpu.make_async_copy(fresh_v.at[:, at, :], fresh_h.at[:, at, :], out_sem.at[step]).wait()


def on_device(
    video_tokens, modulation, project_weight, output_weight, norm_gains,
    text_cache, text_count, video_keep, patch_order, stale_cache,
):
    rows, width = video_tokens.shape
    patch, local = stale_cache.shape[1:]
    hd = norm_gains.shape[1]
    heads = local // hd
    text_rows = text_cache.shape[1]
    half = local // 2
    sub = rows // CHUNKS
    key_rows = 3 * patch + text_rows
    keep = video_keep.reshape(-1, hd)
    y_steps = 3
    anywhere = pl.BlockSpec(memory_space=pl.ANY)
    dma = pltpu.SemaphoreType.DMA
    vmem = pltpu.VMEM
    return pl.pallas_call(
        kernel,
        out_shape=(
            jax.ShapeDtypeStruct((rows, width), BF16),
            jax.ShapeDtypeStruct((2, patch, local), BF16),
        ),
        in_specs=[anywhere] * 10,
        out_specs=(anywhere, anywhere),
        scratch_shapes=[
            vmem((rows, width), BF16),
            vmem(modulation.shape, F32),
            vmem(project_weight.shape, BF16),
            vmem(output_weight.shape, BF16),
            vmem(norm_gains.shape, F32),
            vmem(text_cache.shape, BF16),
            vmem(keep.shape, jnp.int32),
            vmem(stale_cache.shape, BF16),
            vmem((patch, width), BF16),
            vmem((2, rows, width), BF16),
            vmem((CHUNKS, 4 * sub, width), BF16),
            vmem((2, 2, patch, half), BF16),
            vmem((2, 2, patch, half), BF16),
            vmem((patch, local), BF16),
            vmem((key_rows, local), BF16),
            vmem((key_rows, local), BF16),
            vmem((key_rows, hd), BF16),
            vmem((heads, patch, 2 * hd), F32),
            vmem((patch, local), BF16),
            vmem((patch, width), F32),
            vmem((rows, width), BF16),
            vmem((rows, width), BF16),
            vmem((2, patch, local), BF16),
            vmem((rows, width), BF16),
            pltpu.SMEM(patch_order.shape, jnp.int32),
            pltpu.SMEM(text_count.shape, jnp.int32),
            vmem((2 * patch, hd), BF16),
            vmem((patch, hd), BF16),
            vmem((patch, hd), BF16),
            vmem((2, CHUNKS, 2 * sub, hd), BF16),
            vmem((2, CHUNKS, 2 * sub, hd), BF16),
            vmem((2, CHUNKS, 8, 2 * sub), F32),
            vmem((2, CHUNKS, 8, 2 * sub), F32),
            dma((11 + 2 * CHUNKS,)),
            dma((CHUNKS,)),
            dma((CHUNKS,)),
            dma((2, CHUNKS)),
            dma((2, CHUNKS)),
            dma((2, CHUNKS)),
            dma((2, CHUNKS)),
            dma((2, 2, heads // 2)),
            dma((2, 2, heads // 2)),
            dma((y_steps,)),
            dma((y_steps,)),
            dma((2 + y_steps,)),
            dma((2, CHUNKS)),
            dma((2, CHUNKS)),
            dma((2, CHUNKS)),
            dma((2, CHUNKS)),
            pltpu.SemaphoreType.REGULAR,
            pltpu.SemaphoreType.REGULAR,
        ],
        compiler_params=pltpu.CompilerParams(
            collective_id=0, has_side_effects=True, vmem_limit_bytes=60 * 1024 * 1024
        ),
        name="patch_attention",
    )(
        patch_order, text_count, video_tokens, modulation, project_weight, output_weight,
        norm_gains, text_cache, keep, stale_cache,
    )


def solution(mesh):
    placed = (
        P(("groups", "section", "head"), None),
        P("groups", None),
        P(None, None, "head"),
        P("head", None),
        P(),
        P(None, "groups", "head"),
        P("groups"),
        P("groups"),
        P("groups"),
        P(None, ("groups", "section"), "head"),
    )
    return jax.shard_map(
        on_device,
        mesh=mesh,
        in_specs=placed,
        out_specs=(P(("groups", "section", "head"), None), P(None, ("groups", "section"), "head")),
        check_vma=False,
    )
```
